8 devices in a mesh: data: 1 (over z), ys: 2 (over y), xs: 4 (over x, core).
Axes of the slice: x: 2, y: 2, z: 1, core: 2. Of those that a mesh axis runs over, the one named last changes fastest.
Arguments:
- field: float32 [8, 128, 128, 40, 20], P('data', 'xs', 'ys')
- spec_real: float32 [2, 16, 16, 8, 20, 20], replicated
- spec_imag: float32 [2, 16, 16, 8, 20, 20], replicated
- mix_weight: float32 [2, 20, 20], replicated
- bias: float32 [2, 20], replicated
Outputs:
- output: float32 [8, 128, 128, 40, 20], P('data', 'xs', 'ys')
All inputs are finite; a program needn't handle non-finite values.
Results may differ from the reference program's by a relative error of at most 0.001.
Values are sent between devices in bfloat16 or wider.
A program may use at most 1 GiB of HBM per device.

```python
import jax
import jax.numpy as jnp
from jax import lax

PART_BATCH = 8
GRID_X = 128
GRID_Y = 128
GRID_Z = 40
WIDTH = 20
MODES = 8
LAYERS = 2


def spread_modes(kept, first):
    dims = kept.shape
    gap_x = dims[:first] + (GRID_X - 2 * MODES,) + dims[first + 1:]
    full_x = jnp.concatenate([lax.slice_in_dim(kept, 0, MODES, axis=first), jnp.zeros(gap_x, kept.dtype), lax.slice_in_dim(kept, MODES, 2 * MODES, axis=first)], axis=first)
    dims = full_x.shape
    gap_y = dims[:first + 1] + (GRID_Y - 2 * MODES,) + dims[first + 2:]
    full_y = jnp.concatenate([lax.slice_in_dim(full_x, 0, MODES, axis=first + 1), jnp.zeros(gap_y, kept.dtype), lax.slice_in_dim(full_x, MODES, 2 * MODES, axis=first + 1)], axis=first + 1)
    dims = full_y.shape
    gap_z = dims[:first + 2] + (GRID_Z // 2 + 1 - MODES,) + dims[first + 3:]
    return jnp.concatenate([full_y, jnp.zeros(gap_z, kept.dtype)], axis=first + 2)


def setup_inputs(seed: int = 0, part: int = 0) -> dict:
    part_keys = jax.random.split(jax.random.fold_in(jax.random.key(seed), part), 3)
    shared_keys = jax.random.split(jax.random.key(seed + 1), 4)
    kept_shape = (PART_BATCH, 2 * MODES, 2 * MODES, MODES, WIDTH)
    coef_scale = 0.25 * MODES ** -1.5
    kept = lax.complex(jax.random.normal(part_keys[0], kept_shape, jnp.float32), jax.random.normal(part_keys[1], kept_shape, jnp.float32)) * coef_scale
    smooth = jnp.fft.irfftn(spread_modes(kept, 1), s=(GRID_X, GRID_Y, GRID_Z), axes=(1, 2, 3), norm='forward')
    noise = 0.3 * jax.random.normal(part_keys[2], (PART_BATCH, GRID_X, GRID_Y, GRID_Z, WIDTH), jnp.float32)
    kernel_shape = (LAYERS, 2 * MODES, 2 * MODES, MODES, WIDTH, WIDTH)
    kernel_scale = (2.0 * WIDTH) ** -0.5
    return dict(
        field=smooth + noise,
        spec_real=kernel_scale * jax.random.normal(shared_keys[0], kernel_shape, jnp.float32),
        spec_imag=kernel_scale * jax.random.normal(shared_keys[1], kernel_shape, jnp.float32),
        mix_weight=WIDTH ** -0.5 * jax.random.normal(shared_keys[2], (LAYERS, WIDTH, WIDTH), jnp.float32),
        bias=0.5 * jax.random.normal(shared_keys[3], (LAYERS, WIDTH), jnp.float32),
    )


def spectral_conv(sample, kernel):
    spec = jnp.fft.rfftn(sample, axes=(0, 1, 2))
    kept_x = jnp.concatenate([spec[:MODES], spec[GRID_X - MODES:]], axis=0)
    kept = jnp.concatenate([kept_x[:, :MODES], kept_x[:, GRID_Y - MODES:]], axis=1)[:, :, :MODES]
    mixed = jnp.einsum('abci,abcio->abco', kept, kernel)
    return jnp.fft.irfftn(spread_modes(mixed, 0), s=(GRID_X, GRID_Y, GRID_Z), axes=(0, 1, 2))


def reference(field, spec_real, spec_imag, mix_weight, bias):
    def layer_step(carry, weights):
        real_part, imag_part, w_mix, b_vec = weights
        kernel = lax.complex(real_part, imag_part)
        spectral = lax.map(lambda sample: spectral_conv(sample, kernel), carry)
        pointwise = jnp.dot(carry, w_mix, preferred_element_type=jnp.float32)
        return jax.nn.gelu(spectral + pointwise + b_vec, approximate=True), None

    final_field, unused = lax.scan(layer_step, field, (spec_real, spec_imag, mix_weight, bias))
    return final_field
```

```python
import functools
import math

import jax
import jax.numpy as jnp
import numpy as np
from jax import lax
from jax.experimental import pallas as pl
from jax.experimental.pallas import tpu as pltpu
from jax.sharding import PartitionSpec as P

F32 = jnp.float32
BF16 = jnp.bfloat16
LANES = 256
CHUNKS = 2
PACK = 384


def split_xla(v):
    hi = lax.reduce_precision(v, 8, 7)
    rest = v - hi
    mid = lax.reduce_precision(rest, 8, 7)
    return hi.astype(BF16), mid.astype(BF16), (rest - mid).astype(BF16)


def split_np(v):
    v = np.asarray(v, np.float32)
    hi = v.astype(BF16)
    rest = v - hi.astype(np.float32)
    mid = rest.astype(BF16)
    return hi, mid, (rest - mid.astype(np.float32)).astype(BF16)


def split3(v):
    hi = v.astype(BF16)
    rest = v - hi.astype(F32)
    mid = rest.astype(BF16)
    return hi, mid, (rest - mid.astype(F32)).astype(BF16)


def dot(a, b):
    return jnp.dot(a, b, preferred_element_type=F32)


def dot6(a, b):
    return (dot(a[2], b[0]) + dot(a[1], b[1]) + dot(a[0], b[2])) + (dot(a[1], b[0]) + dot(a[0], b[1])) + dot(a[0], b[0])


def six_rows(s):
    return jnp.concatenate([s[0], s[0], s[0], s[1], s[1], s[2]], axis=0)


def six_cols(s, xp=jnp):
    return xp.concatenate([s[0], s[1], s[2], s[0], s[1], s[0]], axis=1)


def lane_map(modes):
    lanes = {}
    for k in range(modes):
        for j in range(2 * modes):
            lanes[k, j] = k * 2 * modes + j
    for k in range(modes):
        lanes[k, 2 * modes] = 128 + k
    for j in range(2 * modes + 1):
        lanes[modes, j] = 128 + modes + j
    return lanes


def tables(modes, grid_x, grid_y, grid_z, x_loc, y_loc, col_devs, row_devs):
    lanes = lane_map(modes)
    used = np.zeros(LANES)
    k_of = np.zeros(LANES)
    j_of = np.zeros(LANES, np.int64)
    for (k, j), lane in lanes.items():
        used[lane], k_of[lane], j_of[lane] = 1.0, k, j
    u = np.arange(x_loc // 2) - (x_loc - 1) / 2.0
    ang = 2 * np.pi * u[:, None] * k_of[None, :] / grid_x
    cos_u, sin_u = np.cos(ang) * used, np.sin(ang) * used
    centre = np.arange(col_devs) * x_loc + (x_loc - 1) / 2.0
    ang = 2 * np.pi * centre[:, None] * k_of[None, :] / grid_x
    p, q = np.cos(ang) * used, np.sin(ang) * used
    y = np.arange(grid_y)
    freq = np.where(j_of <= modes, j_of, j_of - modes)
    ang = 2 * np.pi * ((y[:, None] * freq[None, :]) % grid_y) / grid_y
    trig_y = (np.where(j_of <= modes, np.cos(ang), np.sin(ang)) * used).reshape(row_devs, y_loc, LANES)
    z = np.arange(grid_z)
    kz = np.arange(modes)
    ang = 2 * np.pi * ((z[:, None] * kz[None, :]) % grid_z) / grid_z
    trig_z = np.concatenate([np.cos(ang), np.sin(ang)], axis=1)
    weight = np.where(kz == 0, 1.0, 2.0) / (grid_x * grid_y * grid_z)
    inv_z = trig_z * np.concatenate([weight, weight])[None, :]
    fwd2 = split_np(np.kron(np.eye(2), trig_z.T))
    zero = np.zeros_like(fwd2[0])
    z_fwd = np.concatenate([
        np.concatenate([fwd2[0], fwd2[0], fwd2[0]], axis=1),
        np.concatenate([fwd2[1], fwd2[1], zero], axis=1),
        np.concatenate([fwd2[2], zero, zero], axis=1)], axis=0)
    z_inv = six_cols(split_np(np.kron(np.eye(2), inv_z)), np)
    count = 2 * modes
    sign = np.zeros((2 * count * count, PACK), np.float32)
    where_a = lambda lane: lane if lane < 128 else 128 + lane
    where_b = lambda lane: 128 + lane if lane < 128 else 192 + lane
    for ix in range(count):
        sx, kx = (1, ix) if ix < modes else (-1, count - ix)
        for iy in range(count):
            sy, ky = (1, iy) if iy < modes else (-1, count - iy)
            re = ix * count + iy
            im = re + count * count
            sign[re, where_a(lanes[kx, ky])] += 1
            if kx and ky:
                sign[re, where_b(lanes[kx, modes + ky])] -= sx * sy
            if kx:
                sign[im, where_b(lanes[kx, ky])] -= sx
            if ky:
                sign[im, where_a(lanes[kx, modes + ky])] -= sy
    f32 = lambda a: np.asarray(a, np.float32)
    return dict(cos_u=f32(cos_u), sin_u=f32(sin_u), pq=f32(np.stack([p, q], axis=1)), trig_y=f32(trig_y),
                z_fwd=z_fwd, z_inv=z_inv, to_trig=sign.astype(BF16), to_modes=sign.T.astype(BF16))


def forward_rows(v, z_fwd_ref, zs_ref, side, pair):
    y = dot(z_fwd_ref[...], jnp.concatenate(split3(v), axis=0))
    rows = y.shape[0] // 3
    zs_ref[side, pair * rows:(pair + 1) * rows, :] = y[:rows] + (y[rows:2 * rows] + y[2 * rows:])


def forward_xy(g, zs_ref, xy_ref, acc_ref):
    plus, minus = zs_ref[0], zs_ref[1]
    for part, v in enumerate((plus + minus, plus - minus)):
        new = dot6(split3(v), [xy_ref[part, t, g] for t in range(3)])

        @pl.when(g == 0)
        def _():
            acc_ref[part] = new

        @pl.when(g > 0)
        def _():
            acc_ref[part] += new


def forward_flush(acc_ref, pq_ref, rows_ref, out_ref, width, trigs):
    p, q = pq_ref[0:1], pq_ref[1:2]
    even, odd = acc_ref[0], acc_ref[1]
    a = p * even - q * odd
    b = q * even + p * odd
    tail = a[:, 128:] + pltpu.roll(b[:, 128:], 64, 1)
    packed = jnp.concatenate([a[:, :128], b[:, :128], tail], axis=1)
    rows_ref[...] = packed.reshape(width, trigs, PACK)
    half = trigs // 2
    for t in range(trigs):
        out_ref[t % half, 0, (t // half) * width:(t // half + 1) * width, :] = rows_ref[:, t, :]


def forward_kernel(width, trigs, p_ref, q_ref, z_fwd_ref, xy_ref, pq_ref, out_ref, zs_ref, acc_ref, rows_ref):
    g = pl.program_id(1)
    count = p_ref.shape[1]
    for side, ref in enumerate((p_ref, q_ref)):
        order = range(count) if side == 0 else range(count - 1, -1, -1)
        for pair in range(width // 2):
            v = jnp.concatenate([ref[0, i, 2 * pair:2 * pair + 2].reshape(-1, ref.shape[4]) for i in order], axis=1)
            forward_rows(v, z_fwd_ref, zs_ref, side, pair)
    forward_xy(g, zs_ref, xy_ref, acc_ref)

    @pl.when(g == pl.num_programs(1) - 1)
    def _():
        forward_flush(acc_ref, pq_ref, rows_ref, out_ref, width, trigs)


def inverse_xy(g, coef_ref, pq_ref, rows_ref, gs_ref, xyt_ref, sp_ref, width, trigs):
    @pl.when(g == 0)
    def _():
        half = trigs // 2
        for t in range(trigs):
            rows_ref[:, t, :] = coef_ref[t % half, 0, (t // half) * width:(t // half + 1) * width, :]
        packed = rows_ref[...].reshape(width * trigs, PACK)
        p, q = pq_ref[0:1], pq_ref[1:2]
        tail = packed[:, 256:]
        a = jnp.concatenate([packed[:, :128], tail], axis=1)
        b = jnp.concatenate([packed[:, 128:256], pltpu.roll(tail, 64, 1)], axis=1)
        for part, v in enumerate((p * a + q * b, p * b - q * a)):
            for t, s in enumerate(split3(v)):
                gs_ref[part, t] = s

    even, odd = [dot6([gs_ref[part, t] for t in range(3)], [xyt_ref[part, t, g] for t in range(3)]) for part in range(2)]
    for side, v in enumerate((even + odd, even - odd)):
        for t, s in enumerate(split3(v)):
            sp_ref[side, t] = s


def layer_side(side, load, mix_ref, z_inv_ref, bias_ref, sp_ref, u_ref, width, trigs, grid_z, emit):
    for tile in range(grid_z // 8):
        v = load(tile)
        y = dot(mix_ref[...], six_rows(split3(v)))
        u_ref[:, tile * 8:(tile + 1) * 8, :] = y.reshape(width, 8, LANES)
    for pair in range(width // 2):
        rows = slice(pair * 2 * trigs, (pair + 1) * 2 * trigs)
        y = dot(z_inv_ref[...], six_rows([sp_ref[side, t, rows, :] for t in range(3)]))
        size = 2 * grid_z
        bias = bias_ref[pair * size:(pair + 1) * size, :]
        h = y + (u_ref[2 * pair:2 * pair + 2].reshape(size, LANES) + jnp.concatenate([bias, bias], axis=1))
        emit(pair, jax.nn.gelu(h, approximate=True))


def middle_kernel(width, trigs, grid_z, p_ref, q_ref, coef_ref, mix_ref, z_inv_ref, bias_ref, z_fwd_ref, xy_ref, xyt_ref, pq_ref,
                  v_ref, out_ref, rows_ref, gs_ref, sp_ref, u_ref, zs_ref, acc_ref):
    g = pl.program_id(1)
    count = p_ref.shape[1]
    inverse_xy(g, coef_ref, pq_ref, rows_ref, gs_ref, xyt_ref, sp_ref, width, trigs)
    for side, ref in enumerate((p_ref, q_ref)):
        order = range(count) if side == 0 else range(count - 1, -1, -1)

        def load(tile):
            return jnp.concatenate([ref[0, i, :, tile * 8:(tile + 1) * 8, :].reshape(8 * width, -1) for i in order], axis=1)

        def emit(pair, v):
            size = 2 * grid_z
            v_ref[0, 0, side, pair * size:(pair + 1) * size, :] = v
            forward_rows(v, z_fwd_ref, zs_ref, side, pair)

        layer_side(side, load, mix_ref, z_inv_ref, bias_ref, sp_ref, u_ref, width, trigs, grid_z, emit)
    forward_xy(g, zs_ref, xy_ref, acc_ref)

    @pl.when(g == pl.num_programs(1) - 1)
    def _():
        forward_flush(acc_ref, pq_ref, rows_ref, out_ref, width, trigs)


def last_kernel(width, trigs, grid_z, v_ref, coef_ref, mix_ref, z_inv_ref, bias_ref, xyt_ref, pq_ref,
                out_ref, rows_ref, gs_ref, sp_ref, u_ref):
    g = pl.program_id(1)
    y_loc = out_ref.shape[4]
    count = LANES // y_loc
    inverse_xy(g, coef_ref, pq_ref, rows_ref, gs_ref, xyt_ref, sp_ref, width, trigs)
    for side in range(2):
        def load(tile):
            v = v_ref[0, 0, side].reshape(width, grid_z, LANES)[:, tile * 8:(tile + 1) * 8, :]
            return v.reshape(width * 8, LANES)

        def emit(pair, v):
            for i in range(count):
                x = count * g + i if side == 0 else out_ref.shape[1] - 1 - count * g - i
                out_ref[0, x, 2 * pair:2 * pair + 2] = v[:, i * y_loc:(i + 1) * y_loc].reshape(2, grid_z, y_loc)

        layer_side(side, load, mix_ref, z_inv_ref, bias_ref, sp_ref, u_ref, width, trigs, grid_z, emit)


def mix_kernel(width, in_ref, re_ref, im_ref, to_modes_ref, to_trig_ref, out_ref, f_ref, t_ref):
    batch, rows, _ = in_ref.shape
    n = re_ref.shape[2]
    f_ref[...] = sum(dot(s, to_modes_ref[...]) for s in split3(in_ref[...].reshape(batch * rows, PACK))[::-1]).reshape(batch, rows, 2 * n)

    def one(b, carry):
        f_cos, f_sin = f_ref[b, :width, :], f_ref[b, width:, :]
        s_re = f_cos[:, :n] + f_sin[:, n:]
        s_im = f_cos[:, n:] - f_sin[:, :n]
        t_re = jnp.zeros((width, n), F32)
        t_im = jnp.zeros((width, n), F32)
        for c in range(width):
            w_re, w_im = re_ref[c], im_ref[c]
            a, d = s_re[c:c + 1], s_im[c:c + 1]
            t_re += a * w_re - d * w_im
            t_im += a * w_im + d * w_re
        t_ref[b, :width, :] = jnp.concatenate([t_re, t_im], axis=1)
        t_ref[b, width:, :] = jnp.concatenate([-t_im, t_re], axis=1)
        return carry

    lax.fori_loop(0, batch, one, 0)
    out = sum(dot(s, to_trig_ref[...]) for s in split3(t_ref[...].reshape(batch * rows, 2 * n))[::-1])
    out_ref[...] = out.reshape(batch, rows, PACK)


def full(shape):
    return pl.BlockSpec(shape, lambda *_: (0,) * len(shape))


def params(mib, grid=2):
    return pltpu.CompilerParams(dimension_semantics=('arbitrary',) * grid, vmem_limit_bytes=mib * 2 ** 20)


def solution(mesh):
    row_devs = mesh.shape['ys']
    col_devs = mesh.shape['xs']

    def local_layers(field, spec_real, spec_imag, mix_weight, bias):
        batch, x_loc, y_loc, grid_z, width = field.shape
        layers = spec_real.shape[0]
        modes = spec_real.shape[3]
        trigs = 2 * modes
        rows = width * trigs
        count = LANES // y_loc
        groups = x_loc // (2 * count)
        t = tables(modes, x_loc * col_devs, y_loc * row_devs, grid_z, x_loc, y_loc, col_devs, row_devs)
        x_index = lax.axis_index('xs')
        y_index = lax.axis_index('ys')
        trig_y = lax.dynamic_index_in_dim(jnp.asarray(t['trig_y']), y_index, 0, keepdims=False)
        pq = lax.dynamic_index_in_dim(jnp.asarray(t['pq']), x_index, 0, keepdims=False)
        trig_x = jnp.stack([jnp.asarray(t['cos_u']), jnp.asarray(t['sin_u'])])
        xy = (trig_x[:, :, None, :] * trig_y[None, None]).reshape(2, groups, LANES, LANES)
        xy = jnp.stack(split_xla(xy), axis=1)
        xyt = jnp.swapaxes(xy, 3, 4)
        z_fwd, z_inv = jnp.asarray(t['z_fwd']), jnp.asarray(t['z_inv'])
        to_modes, to_trig = jnp.asarray(t['to_modes']), jnp.asarray(t['to_trig'])
        eye = jnp.eye(8, dtype=F32)
        mix = [six_cols(split_xla(jnp.einsum('cd,zw->dzcw', mix_weight[l], eye, precision=lax.Precision.HIGHEST).reshape(8 * width, 8 * width))) for l in range(layers)]
        bias_rows = jnp.broadcast_to(bias[:, :, None, None], (layers, width, grid_z, 128)).reshape(layers, width * grid_z, 128)
        kz = y_index * col_devs + x_index

        def own(w):
            w = lax.dynamic_index_in_dim(w, kz, 3, keepdims=False)
            return jnp.transpose(w, (0, 3, 4, 1, 2)).reshape(layers, width, width, trigs * trigs)

        real_w, imag_w = own(spec_real), own(spec_imag)

        native = jnp.transpose(field, (0, 1, 4, 3, 2))
        chunk = batch // CHUNKS
        xy_spec = full(xy.shape)
        spectrum = jax.ShapeDtypeStruct((modes, chunk, 2 * width, PACK), F32)
        spec_block = pl.BlockSpec((modes, 1, 2 * width, PACK), lambda b, g: (0, b, 0, 0))
        packed = jax.ShapeDtypeStruct((chunk, groups, 2, width * grid_z, LANES), F32)
        packed_block = pl.BlockSpec((1, 1, 2, width * grid_z, LANES), lambda b, g: (b, g, 0, 0, 0))
        rows_scr = pltpu.VMEM((width, trigs, PACK), F32)
        zs_scr = pltpu.VMEM((2, rows, LANES), F32)
        acc_scr = pltpu.VMEM((2, rows, LANES), F32)
        gs_scr = pltpu.VMEM((2, 3, rows, LANES), BF16)
        sp_scr = pltpu.VMEM((2, 3, rows, LANES), BF16)
        u_scr = pltpu.VMEM((width, grid_z, LANES), F32)

        def field_blocks(first):
            shape = (1, count, width, grid_z, y_loc)
            return [pl.BlockSpec(shape, lambda b, g: (first + b, g, 0, 0, 0)),
                    pl.BlockSpec(shape, lambda b, g: (first + b, 2 * groups - 1 - g, 0, 0, 0))]

        def cost(us):
            return pl.CostEstimate(flops=int(us * chunk * 4e7), bytes_accessed=chunk * 13 * 2 ** 20, transcendentals=0)

        def forward(first):
            return pl.pallas_call(
                functools.partial(forward_kernel, width, trigs), grid=(chunk, groups),
                in_specs=field_blocks(first) + [full(z_fwd.shape), xy_spec, full(pq.shape)],
                out_specs=spec_block, out_shape=spectrum, scratch_shapes=[zs_scr, acc_scr, rows_scr],
                compiler_params=params(56), cost_estimate=cost(8), name='forward')(native, native, z_fwd, xy, pq)

        def middle(first, coef):
            return pl.pallas_call(
                functools.partial(middle_kernel, width, trigs, grid_z), grid=(chunk, groups),
                in_specs=field_blocks(first) + [spec_block, full(mix[0].shape), full(z_inv.shape), full(bias_rows.shape[1:]), full(z_fwd.shape), xy_spec, xy_spec, full(pq.shape)],
                out_specs=[packed_block, spec_block], out_shape=[packed, spectrum],
                scratch_shapes=[rows_scr, gs_scr, sp_scr, u_scr, zs_scr, acc_scr],
                compiler_params=params(60), cost_estimate=cost(22), name='middle')(
                    native, native, coef, mix[0], z_inv, bias_rows[0], z_fwd, xy, xyt, pq)

        def last(first, v, coef, out):
            specs = [packed_block, spec_block, full(mix[1].shape), full(z_inv.shape), full(bias_rows.shape[1:]), xy_spec, full(pq.shape)]
            args = [v, coef, mix[1], z_inv, bias_rows[1], xyt, pq]
            kernel = functools.partial(last_kernel, width, trigs, grid_z)
            if out is not None:
                specs, args = [pl.BlockSpec(memory_space=pl.ANY)] + specs, [out] + args
            body = kernel if out is None else lambda unused, *refs: kernel(*refs)
            return pl.pallas_call(
                body, grid=(chunk, groups), in_specs=specs,
                out_specs=pl.BlockSpec((1, x_loc, width, grid_z, y_loc), lambda b, g: (first + b, 0, 0, 0, 0)),
                out_shape=jax.ShapeDtypeStruct(native.shape, F32), scratch_shapes=[rows_scr, gs_scr, sp_scr, u_scr],
                input_output_aliases={} if out is None else {0: 0},
                compiler_params=params(60), cost_estimate=cost(12), name='last')(*args)

        mixing = pl.pallas_call(
            functools.partial(mix_kernel, width), out_shape=jax.ShapeDtypeStruct((chunk, 2 * width, PACK), F32),
            scratch_shapes=[pltpu.VMEM((chunk, 2 * width, 2 * trigs * trigs), F32)] * 2, cost_estimate=cost(0.3),
            compiler_params=pltpu.CompilerParams(vmem_limit_bytes=32 * 2 ** 20), name='mixing')

        def gather_sum(partial):
            return lax.psum_scatter(partial, ('ys', 'xs'), scatter_dimension=0, tiled=False)

        def spread(own_sum, layer):
            mixed = mixing(own_sum, real_w[layer], imag_w[layer], to_modes, to_trig)
            return lax.all_gather(mixed, ('ys', 'xs'), axis=0, tiled=False)

        parts = [gather_sum(forward(i * chunk)) for i in range(CHUNKS)]
        coefs = [spread(part, 0) for part in parts]
        done = [middle(i * chunk, coef) for i, coef in enumerate(coefs)]
        parts = [gather_sum(partial) for v, partial in done]
        coefs = [spread(part, 1) for part in parts]
        out = None
        for i in range(CHUNKS):
            out = last(i * chunk, done[i][0], coefs[i], out)
        return jnp.transpose(out, (0, 1, 4, 3, 2))

    field_spec = P('data', 'xs', 'ys', None, None)
    return jax.shard_map(local_layers, mesh=mesh, in_specs=(field_spec, P(), P(), P(), P()), out_specs=field_spec, check_vma=False)
```

```python
import functools
import math

import jax
import jax.numpy as jnp
import numpy as np
from jax import lax
from jax.experimental import pallas as pl
from jax.experimental.pallas import tpu as pltpu
from jax.sharding import PartitionSpec as P

F32 = jnp.float32
BF16 = jnp.bfloat16
LANES = 256
PACK = 384


def split_xla(v):
    hi = lax.reduce_precision(v, 8, 7)
    rest = v - hi
    mid = lax.reduce_precision(rest, 8, 7)
    return hi.astype(BF16), mid.astype(BF16), (rest - mid).astype(BF16)


def split_np(v):
    v = np.asarray(v, np.float32)
    hi = v.astype(BF16)
    rest = v - hi.astype(np.float32)
    mid = rest.astype(BF16)
    return hi, mid, (rest - mid.astype(np.float32)).astype(BF16)


def split3(v):
    hi = v.astype(BF16)
    rest = v - hi.astype(F32)
    mid = rest.astype(BF16)
    return hi, mid, (rest - mid.astype(F32)).astype(BF16)


def dot(a, b):
    return jnp.dot(a, b, preferred_element_type=F32)


def dot6(a, b):
    return (dot(a[2], b[0]) + dot(a[1], b[1]) + dot(a[0], b[2])) + (dot(a[1], b[0]) + dot(a[0], b[1])) + dot(a[0], b[0])


def six_rows(s):
    return jnp.concatenate([s[0], s[0], s[0], s[1], s[1], s[2]], axis=0)


def six_cols(s, xp=jnp):
    return xp.concatenate([s[0], s[1], s[2], s[0], s[1], s[0]], axis=1)


def lane_map(modes):
    lanes = {}
    for k in range(modes):
        for j in range(2 * modes):
            lanes[k, j] = k * 2 * modes + j
    for k in range(modes):
        lanes[k, 2 * modes] = 128 + k
    for j in range(2 * modes + 1):
        lanes[modes, j] = 128 + modes + j
    return lanes


def tables(modes, grid_x, grid_y, grid_z, x_loc, y_loc, col_devs, row_devs):
    lanes = lane_map(modes)
    used = np.zeros(LANES)
    k_of = np.zeros(LANES)
    j_of = np.zeros(LANES, np.int64)
    for (k, j), lane in lanes.items():
        used[lane], k_of[lane], j_of[lane] = 1.0, k, j
    u = np.arange(x_loc // 2) - (x_loc - 1) / 2.0
    ang = 2 * np.pi * u[:, None] * k_of[None, :] / grid_x
    cos_u, sin_u = np.cos(ang) * used, np.sin(ang) * used
    centre = np.arange(col_devs) * x_loc + (x_loc - 1) / 2.0
    ang = 2 * np.pi * centre[:, None] * k_of[None, :] / grid_x
    p, q = np.cos(ang) * used, np.sin(ang) * used
    y = np.arange(grid_y)
    freq = np.where(j_of <= modes, j_of, j_of - modes)
    ang = 2 * np.pi * ((y[:, None] * freq[None, :]) % grid_y) / grid_y
    trig_y = (np.where(j_of <= modes, np.cos(ang), np.sin(ang)) * used).reshape(row_devs, y_loc, LANES)
    z = np.arange(grid_z)
    kz = np.arange(modes)
    ang = 2 * np.pi * ((z[:, None] * kz[None, :]) % grid_z) / grid_z
    trig_z = np.concatenate([np.cos(ang), np.sin(ang)], axis=1)
    weight = np.where(kz == 0, 1.0, 2.0) / (grid_x * grid_y * grid_z)
    inv_z = trig_z * np.concatenate([weight, weight])[None, :]
    fwd2 = split_np(np.kron(np.eye(2), trig_z.T))
    zero = np.zeros_like(fwd2[0])
    z_fwd = np.concatenate([
        np.concatenate([fwd2[0], fwd2[0], fwd2[0]], axis=1),
        np.concatenate([fwd2[1], fwd2[1], zero], axis=1),
        np.concatenate([fwd2[2], zero, zero], axis=1)], axis=0)
    z_inv = six_cols(split_np(np.kron(np.eye(2), inv_z)), np)
    count = 2 * modes
    sign = np.zeros((2 * count * count, PACK), np.float32)
    where_a = lambda lane: lane if lane < 128 else 128 + lane
    where_b = lambda lane: 128 + lane if lane < 128 else 192 + lane
    for ix in range(count):
        sx, kx = (1, ix) if ix < modes else (-1, count - ix)
        for iy in range(count):
            sy, ky = (1, iy) if iy < modes else (-1, count - iy)
            re = ix * count + iy
            im = re + count * count
            sign[re, where_a(lanes[kx, ky])] += 1
            if kx and ky:
                sign[re, where_b(lanes[kx, modes + ky])] -= sx * sy
            if kx:
                sign[im, where_b(lanes[kx, ky])] -= sx
            if ky:
                sign[im, where_a(lanes[kx, modes + ky])] -= sy
    f32 = lambda a: np.asarray(a, np.float32)
    return dict(cos_u=f32(cos_u), sin_u=f32(sin_u), pq=f32(np.stack([p, q], axis=1)), trig_y=f32(trig_y),
                z_fwd=z_fwd, z_inv=z_inv, to_trig=sign.astype(BF16), to_modes=sign.T.astype(BF16))


def forward_rows(v, z_fwd_ref, zs_ref, ts_ref, side, pair):
    y = dot(z_fwd_ref[...], jnp.concatenate(split3(v), axis=0))
    size = y.shape[0] // 3
    y = y[:size] + (y[size:2 * size] + y[2 * size:])
    rows = slice(pair * size, (pair + 1) * size)
    if side == 0:
        zs_ref[rows, :] = y
        return
    first = zs_ref[rows, :]
    for part, v in enumerate((first + y, first - y)):
        for t, s in enumerate(split3(v)):
            ts_ref[part, t, rows, :] = s


def forward_xy(g, ts_ref, xy_ref, acc_ref):
    @pl.when(g == 0)
    def _():
        acc_ref[...] = jnp.zeros_like(acc_ref)

    for part in range(2):
        acc_ref[part] += dot6([ts_ref[part, t] for t in range(3)], [xy_ref[part, t, g] for t in range(3)])


def forward_flush(acc_ref, pq_ref, rows_ref, out_ref, width, trigs):
    p, q = pq_ref[0:1], pq_ref[1:2]
    even, odd = acc_ref[0], acc_ref[1]
    a = p * even - q * odd
    b = q * even + p * odd
    tail = a[:, 128:] + pltpu.roll(b[:, 128:], 64, 1)
    packed = jnp.concatenate([a[:, :128], b[:, :128], tail], axis=1)
    rows_ref[...] = packed.reshape(width, trigs, PACK)
    half = trigs // 2
    for t in range(trigs):
        out_ref[t % half, 0, (t // half) * width:(t // half + 1) * width, :] = rows_ref[:, t, :]


def forward_kernel(width, trigs, p_ref, q_ref, z_fwd_ref, xy_ref, pq_ref, out_ref, zs_ref, ts_ref, acc_ref, rows_ref):
    g = pl.program_id(1)
    count = p_ref.shape[1]
    for side, ref in enumerate((p_ref, q_ref)):
        order = range(count) if side == 0 else range(count - 1, -1, -1)
        for pair in range(width // 2):
            v = jnp.concatenate([ref[0, i, 2 * pair:2 * pair + 2].reshape(-1, ref.shape[4]) for i in order], axis=1)
            forward_rows(v, z_fwd_ref, zs_ref, ts_ref, side, pair)
    forward_xy(g, ts_ref, xy_ref, acc_ref)

    @pl.when(g == pl.num_programs(1) - 1)
    def _():
        forward_flush(acc_ref, pq_ref, rows_ref, out_ref, width, trigs)


def inverse_xy(g, coef_ref, pq_ref, rows_ref, gs_ref, xyt_ref, sp_ref, width, trigs):
    @pl.when(g == 0)
    def _():
        half = trigs // 2
        for t in range(trigs):
            rows_ref[:, t, :] = coef_ref[t % half, 0, (t // half) * width:(t // half + 1) * width, :]
        packed = rows_ref[...].reshape(width * trigs, PACK)
        p, q = pq_ref[0:1], pq_ref[1:2]
        tail = packed[:, 256:]
        a = jnp.concatenate([packed[:, :128], tail], axis=1)
        b = jnp.concatenate([packed[:, 128:256], pltpu.roll(tail, 64, 1)], axis=1)
        for part, v in enumerate((p * a + q * b, p * b - q * a)):
            for t, s in enumerate(split3(v)):
                gs_ref[part, t] = s

    for part in range(2):
        sp_ref[part] = dot6([gs_ref[part, t] for t in range(3)], [xyt_ref[part, t, g] for t in range(3)])


def layer_side(side, load, mix_ref, z_inv_ref, bias_ref, sp_ref, u_ref, width, trigs, grid_z, emit):
    for tile in range(grid_z // 8):
        v = load(tile)
        y = dot(mix_ref[...], six_rows(split3(v)))
        u_ref[:, tile * 8:(tile + 1) * 8, :] = y.reshape(width, 8, LANES)
    for pair in range(width // 2):
        rows = slice(pair * 2 * trigs, (pair + 1) * 2 * trigs)
        even, odd = sp_ref[0, rows, :], sp_ref[1, rows, :]
        y = dot(z_inv_ref[...], six_rows(split3(even + odd if side == 0 else even - odd)))
        size = 2 * grid_z
        bias = bias_ref[pair * size:(pair + 1) * size, :]
        h = y + (u_ref[2 * pair:2 * pair + 2].reshape(size, LANES) + jnp.concatenate([bias, bias], axis=1))
        emit(pair, jax.nn.gelu(h, approximate=True))


def middle_kernel(width, trigs, grid_z, p_ref, q_ref, coef_ref, mix_ref, z_inv_ref, bias_ref, z_fwd_ref, xy_ref, xyt_ref, pq_ref,
                  v_ref, out_ref, rows_ref, gs_ref, sp_ref, u_ref, zs_ref, ts_ref, acc_ref):
    g = pl.program_id(1)
    count = p_ref.shape[1]
    inverse_xy(g, coef_ref, pq_ref, rows_ref, gs_ref, xyt_ref, sp_ref, width, trigs)
    for side, ref in enumerate((p_ref, q_ref)):
        order = range(count) if side == 0 else range(count - 1, -1, -1)

        def load(tile):
            return jnp.concatenate([ref[0, i, :, tile * 8:(tile + 1) * 8, :].reshape(8 * width, -1) for i in order], axis=1)

        def emit(pair, v):
            size = 2 * grid_z
            v_ref[0, 0, side, pair * size:(pair + 1) * size, :] = v
            forward_rows(v, z_fwd_ref, zs_ref, ts_ref, side, pair)

        layer_side(side, load, mix_ref, z_inv_ref, bias_ref, sp_ref, u_ref, width, trigs, grid_z, emit)
    forward_xy(g, ts_ref, xy_ref, acc_ref)

    @pl.when(g == pl.num_programs(1) - 1)
    def _():
        forward_flush(acc_ref, pq_ref, rows_ref, out_ref, width, trigs)


def last_kernel(width, trigs, grid_z, v_ref, coef_ref, mix_ref, z_inv_ref, bias_ref, xyt_ref, pq_ref,
                out_ref, rows_ref, gs_ref, sp_ref, u_ref):
    g = pl.program_id(1)
    y_loc = out_ref.shape[4]
    count = LANES // y_loc
    inverse_xy(g, coef_ref, pq_ref, rows_ref, gs_ref, xyt_ref, sp_ref, width, trigs)
    for side in range(2):
        def load(tile):
            v = v_ref[0, 0, side].reshape(width, grid_z, LANES)[:, tile * 8:(tile + 1) * 8, :]
            return v.reshape(width * 8, LANES)

        def emit(pair, v):
            for i in range(count):
                x = count * g + i if side == 0 else out_ref.shape[1] - 1 - count * g - i
                out_ref[0, x, 2 * pair:2 * pair + 2] = v[:, i * y_loc:(i + 1) * y_loc].reshape(2, grid_z, y_loc)

        layer_side(side, load, mix_ref, z_inv_ref, bias_ref, sp_ref, u_ref, width, trigs, grid_z, emit)


def mix_kernel(width, in_ref, re_ref, im_ref, to_modes_ref, to_trig_ref, out_ref, f_ref, t_ref):
    batch, rows, _ = in_ref.shape
    n = re_ref.shape[2]
    f_ref[...] = sum(dot(s, to_modes_ref[...]) for s in split3(in_ref[...].reshape(batch * rows, PACK))[::-1]).reshape(batch, rows, 2 * n)

    def one(b, carry):
        f_cos, f_sin = f_ref[b, :width, :], f_ref[b, width:, :]
        s_re = f_cos[:, :n] + f_sin[:, n:]
        s_im = f_cos[:, n:] - f_sin[:, :n]
        t_re = jnp.zeros((width, n), F32)
        t_im = jnp.zeros((width, n), F32)
        for c in range(width):
            w_re, w_im = re_ref[c], im_ref[c]
            a, d = s_re[c:c + 1], s_im[c:c + 1]
            t_re += a * w_re - d * w_im
            t_im += a * w_im + d * w_re
        t_ref[b, :width, :] = jnp.concatenate([t_re, t_im], axis=1)
        t_ref[b, width:, :] = jnp.concatenate([-t_im, t_re], axis=1)
        return carry

    lax.fori_loop(0, batch, one, 0)
    out = sum(dot(s, to_trig_ref[...]) for s in split3(t_ref[...].reshape(batch * rows, 2 * n))[::-1])
    out_ref[...] = out.reshape(batch, rows, PACK)


def weights_kernel(col_devs, re_ref, im_ref, *refs):
    outs, buf, sem = refs[:-2], refs[-2], refs[-1]
    kz = lax.axis_index('ys') * col_devs + lax.axis_index('xs')
    size = buf.shape[1]
    width, _, n = outs[0].shape
    copies = []
    for i in range(len(outs)):
        ref = re_ref if i % 2 == 0 else im_ref
        copies.append(pltpu.make_async_copy(ref.at[pl.ds(i // 2 * size, size), kz], buf.at[i], sem.at[i]))
        copies[-1].start()
    for i, out in enumerate(outs):
        copies[i].wait()
        for c in range(width):
            out[c] = buf[i, pl.ds(c, n, stride=width), 0, :].T


def full(shape):
    return pl.BlockSpec(shape, lambda *_: (0,) * len(shape))


def params(mib, grid=2):
    return pltpu.CompilerParams(dimension_semantics=('arbitrary',) * grid, vmem_limit_bytes=mib * 2 ** 20)


def solution(mesh):
    row_devs = mesh.shape['ys']
    col_devs = mesh.shape['xs']

    def local_layers(field, spec_real, spec_imag, mix_weight, bias):
        batch, x_loc, y_loc, grid_z, width = field.shape
        layers = spec_real.shape[0]
        modes = spec_real.shape[3]
        trigs = 2 * modes
        rows = width * trigs
        count = LANES // y_loc
        groups = x_loc // (2 * count)
        t = tables(modes, x_loc * col_devs, y_loc * row_devs, grid_z, x_loc, y_loc, col_devs, row_devs)
        x_index = lax.axis_index('xs')
        y_index = lax.axis_index('ys')
        trig_y = lax.dynamic_index_in_dim(jnp.asarray(t['trig_y']), y_index, 0, keepdims=False)
        pq = lax.dynamic_index_in_dim(jnp.asarray(t['pq']), x_index, 0, keepdims=False)
        trig_x = jnp.stack([jnp.asarray(t['cos_u']), jnp.asarray(t['sin_u'])])
        xy = (trig_x[:, :, None, :] * trig_y[None, None]).reshape(2, groups, LANES, LANES)
        xy = jnp.stack(split_xla(xy), axis=1)
        xyt = jnp.swapaxes(xy, 3, 4)
        z_fwd, z_inv = jnp.asarray(t['z_fwd']), jnp.asarray(t['z_inv'])
        to_modes, to_trig = jnp.asarray(t['to_modes']), jnp.asarray(t['to_trig'])
        eye = jnp.eye(8, dtype=F32)
        mix = [six_cols(split_xla(jnp.einsum('cd,zw->dzcw', mix_weight[l], eye, precision=lax.Precision.HIGHEST).reshape(8 * width, 8 * width))) for l in range(layers)]
        bias_rows = jnp.broadcast_to(bias[:, :, None, None], (layers, width, grid_z, 128)).reshape(layers, width * grid_z, 128)
        by_row = lambda w: jnp.transpose(w, (0, 1, 2, 4, 3, 5)).reshape(layers * trigs * trigs * width, modes, 1, width)
        own = pl.pallas_call(
            functools.partial(weights_kernel, col_devs), in_specs=[pl.BlockSpec(memory_space=pl.ANY)] * 2,
            out_shape=[jax.ShapeDtypeStruct((width, width, trigs * trigs), F32)] * (2 * layers),
            scratch_shapes=[pltpu.VMEM((2 * layers, trigs * trigs * width, 1, width), F32), pltpu.SemaphoreType.DMA((2 * layers,))],
            cost_estimate=pl.CostEstimate(flops=400000000, bytes_accessed=2 ** 24, transcendentals=0),
            compiler_params=pltpu.CompilerParams(vmem_limit_bytes=32 * 2 ** 20), name='weights')(by_row(spec_real), by_row(spec_imag))

        native = jnp.transpose(field, (0, 1, 4, 3, 2))
        xy_spec = full(xy.shape)
        packed_block = pl.BlockSpec((1, 1, 2, width * grid_z, LANES), lambda b, g: (b, g, 0, 0, 0))
        rows_scr = pltpu.VMEM((width, trigs, PACK), F32)
        zs_scr = pltpu.VMEM((rows, LANES), F32)
        ts_scr = pltpu.VMEM((2, 3, rows, LANES), BF16)
        acc_scr = pltpu.VMEM((2, rows, LANES), F32)
        gs_scr = pltpu.VMEM((2, 3, rows, LANES), BF16)
        sp_scr = pltpu.VMEM((2, rows, LANES), F32)
        u_scr = pltpu.VMEM((width, grid_z, LANES), F32)

        half, part = batch // 2, batch // 4

        def field_blocks(first):
            shape = (1, count, width, grid_z, y_loc)
            return [pl.BlockSpec(shape, lambda b, g: (first + b, g, 0, 0, 0)),
                    pl.BlockSpec(shape, lambda b, g: (first + b, 2 * groups - 1 - g, 0, 0, 0))]

        def cost(us, n):
            return pl.CostEstimate(flops=int(us * n * 4e7), bytes_accessed=n * 13 * 2 ** 20, transcendentals=0)

        def ordered(kernel, after, specs, args, **settings):
            extra = len(after)
            return pl.pallas_call(lambda *refs: kernel(*refs[extra:]), in_specs=[pl.BlockSpec(memory_space=pl.ANY)] * extra + specs,
                                  **settings)(*after, *args)

        sums = jax.ShapeDtypeStruct((modes, half, 2 * width, PACK), F32)

        def sums_block(at):
            return pl.BlockSpec((modes, 1, 2 * width, PACK), lambda b, g: (0, at + b, 0, 0))

        def forward(first, n, at, into, after):
            return ordered(
                functools.partial(forward_kernel, width, trigs), after if into is None else [into] + after,
                field_blocks(first) + [full(z_fwd.shape), xy_spec, full(pq.shape)], [native, native, z_fwd, xy, pq],
                grid=(n, groups), out_specs=sums_block(at), out_shape=sums, scratch_shapes=[zs_scr, ts_scr, acc_scr, rows_scr],
                input_output_aliases={} if into is None else {0: 0},
                compiler_params=params(56), cost_estimate=cost(8, n), name='forward')

        def middle(first, n, at, coef, into, after):
            return ordered(
                functools.partial(middle_kernel, width, trigs, grid_z), after if into is None else [into] + after,
                field_blocks(first) + [sums_block(at), full(mix[0].shape), full(z_inv.shape), full(bias_rows.shape[1:]), full(z_fwd.shape), xy_spec, xy_spec, full(pq.shape)],
                [native, native, coef, mix[0], z_inv, bias_rows[0], z_fwd, xy, xyt, pq],
                grid=(n, groups), out_specs=[packed_block, sums_block(at)],
                out_shape=[jax.ShapeDtypeStruct((n, groups, 2, width * grid_z, LANES), F32), sums],
                scratch_shapes=[rows_scr, gs_scr, sp_scr, u_scr, zs_scr, ts_scr, acc_scr],
                input_output_aliases={} if into is None else {0: 1},
                compiler_params=params(60), cost_estimate=cost(20, n), name='middle')

        def last(first, n, at, v, coef, out, after):
            first_call = out is None
            return ordered(
                functools.partial(last_kernel, width, trigs, grid_z), after if first_call else [out] + after,
                [packed_block, sums_block(at), full(mix[1].shape), full(z_inv.shape), full(bias_rows.shape[1:]), xy_spec, full(pq.shape)],
                [v, coef, mix[1], z_inv, bias_rows[1], xyt, pq],
                grid=(n, groups), out_specs=pl.BlockSpec((1, x_loc, width, grid_z, y_loc), lambda b, g: (first + b, 0, 0, 0, 0)),
                out_shape=jax.ShapeDtypeStruct(native.shape, F32), scratch_shapes=[rows_scr, gs_scr, sp_scr, u_scr],
                input_output_aliases={} if first_call else {0: 0},
                compiler_params=params(60), cost_estimate=cost(12, n), name='last')

        def mixing(own_sum, layer, after):
            n = own_sum.shape[0]
            args = [own_sum, own[2 * layer], own[2 * layer + 1], to_modes, to_trig]
            return ordered(
                functools.partial(mix_kernel, width), after, [pl.BlockSpec(memory_space=pltpu.VMEM)] * len(args), args,
                out_shape=jax.ShapeDtypeStruct((n, 2 * width, PACK), F32),
                scratch_shapes=[pltpu.VMEM((n, 2 * width, 2 * trigs * trigs), F32)] * 2, cost_estimate=cost(0.5, n),
                compiler_params=pltpu.CompilerParams(vmem_limit_bytes=32 * 2 ** 20), name='mixing')

        def gather_sum(partial):
            return lax.psum_scatter(partial, ('ys', 'xs'), scatter_dimension=0, tiled=False)

        def spread(mixed):
            return lax.all_gather(mixed, ('ys', 'xs'), axis=0, tiled=False)

        sum_a = gather_sum(forward(0, half, 0, None, []))
        fwd_b = forward(half, part, 0, None, [])
        mix_a = mixing(sum_a, 0, [fwd_b])
        coef_a = spread(mix_a)
        fwd_b = forward(half + part, part, part, fwd_b, [mix_a])
        sum_b = gather_sum(fwd_b)
        v_0, mid_a = middle(0, part, 0, coef_a, None, [fwd_b])
        mix_b = mixing(sum_b, 0, [mid_a])
        coef_b = spread(mix_b)
        v_1, mid_a = middle(part, part, part, coef_a, mid_a, [mix_b])
        sum_a = gather_sum(mid_a)
        v_2, mid_b = middle(half, part, 0, coef_b, None, [mid_a])
        mix_a = mixing(sum_a, 1, [mid_b])
        coef_a = spread(mix_a)
        v_3, mid_b = middle(half + part, part, part, coef_b, mid_b, [mix_a])
        sum_b = gather_sum(mid_b)
        out = last(0, part, 0, v_0, coef_a, None, [mid_b])
        mix_b = mixing(sum_b, 1, [out])
        coef_b = spread(mix_b)
        out = last(part, part, part, v_1, coef_a, out, [mix_b])
        out = last(half, part, 0, v_2, coef_b, out, [])
        out = last(half + part, part, part, v_3, coef_b, out, [])
        return jnp.transpose(out, (0, 1, 4, 3, 2))

    field_spec = P('data', 'xs', 'ys', None, None)
    return jax.shard_map(local_layers, mesh=mesh, in_specs=(field_spec, P(), P(), P(), P()), out_specs=field_spec, check_vma=False)
```

```python
import functools
import math

import jax
import jax.numpy as jnp
import numpy as np
from jax import lax
from jax.experimental import pallas as pl
from jax.experimental.pallas import tpu as pltpu
from jax.sharding import PartitionSpec as P

F32 = jnp.float32
BF16 = jnp.bfloat16
LANES = 256
PACK = 384


def split_xla(v):
    hi = lax.reduce_precision(v, 8, 7)
    rest = v - hi
    mid = lax.reduce_precision(rest, 8, 7)
    return hi.astype(BF16), mid.astype(BF16), (rest - mid).astype(BF16)


def split_np(v):
    v = np.asarray(v, np.float32)
    hi = v.astype(BF16)
    rest = v - hi.astype(np.float32)
    mid = rest.astype(BF16)
    return hi, mid, (rest - mid.astype(np.float32)).astype(BF16)


def split3(v):
    hi = v.astype(BF16)
    rest = v - hi.astype(F32)
    mid = rest.astype(BF16)
    return hi, mid, (rest - mid.astype(F32)).astype(BF16)


def dot(a, b):
    return jnp.dot(a, b, preferred_element_type=F32)


def dot6(a, b):
    return (dot(a[2], b[0]) + dot(a[1], b[1]) + dot(a[0], b[2])) + (dot(a[1], b[0]) + dot(a[0], b[1])) + dot(a[0], b[0])


def six_rows(s):
    return jnp.concatenate([s[0], s[0], s[0], s[1], s[1], s[2]], axis=0)


def six_cols(s, xp=jnp):
    return xp.concatenate([s[0], s[1], s[2], s[0], s[1], s[0]], axis=1)


def gelu(h):
    c = math.sqrt(2.0 / math.pi)
    return (0.5 * h) * (1.0 + jnp.tanh(h * (c + (c * 0.044715) * (h * h))))


def lane_map(modes):
    lanes = {}
    for k in range(modes):
        for j in range(2 * modes):
            lanes[k, j] = k * 2 * modes + j
    for k in range(modes):
        lanes[k, 2 * modes] = 128 + k
    for j in range(2 * modes + 1):
        lanes[modes, j] = 128 + modes + j
    return lanes


def tables(modes, grid_x, grid_y, grid_z, x_loc, y_loc, col_devs, row_devs):
    lanes = lane_map(modes)
    used = np.zeros(LANES)
    k_of = np.zeros(LANES)
    j_of = np.zeros(LANES, np.int64)
    for (k, j), lane in lanes.items():
        used[lane], k_of[lane], j_of[lane] = 1.0, k, j
    u = np.arange(x_loc // 2) - (x_loc - 1) / 2.0
    ang = 2 * np.pi * u[:, None] * k_of[None, :] / grid_x
    cos_u, sin_u = np.cos(ang) * used, np.sin(ang) * used
    centre = np.arange(col_devs) * x_loc + (x_loc - 1) / 2.0
    ang = 2 * np.pi * centre[:, None] * k_of[None, :] / grid_x
    p, q = np.cos(ang) * used, np.sin(ang) * used
    y = np.arange(grid_y)
    freq = np.where(j_of <= modes, j_of, j_of - modes)
    ang = 2 * np.pi * ((y[:, None] * freq[None, :]) % grid_y) / grid_y
    trig_y = (np.where(j_of <= modes, np.cos(ang), np.sin(ang)) * used).reshape(row_devs, y_loc, LANES)
    z = np.arange(grid_z)
    kz = np.arange(modes)
    ang = 2 * np.pi * ((z[:, None] * kz[None, :]) % grid_z) / grid_z
    trig_z = np.concatenate([np.cos(ang), np.sin(ang)], axis=1)
    weight = np.where(kz == 0, 1.0, 2.0) / (grid_x * grid_y * grid_z)
    inv_z = trig_z * np.concatenate([weight, weight])[None, :]
    fwd2 = split_np(np.kron(np.eye(2), trig_z.T))
    zero = np.zeros_like(fwd2[0])
    z_fwd = np.concatenate([
        np.concatenate([fwd2[0], fwd2[0], fwd2[0]], axis=1),
        np.concatenate([fwd2[1], fwd2[1], zero], axis=1),
        np.concatenate([fwd2[2], zero, zero], axis=1)], axis=0)
    z_inv = six_cols(split_np(np.kron(np.eye(2), inv_z)), np)
    count = 2 * modes
    sign = np.zeros((2 * count * count, PACK), np.float32)
    where_a = lambda lane: lane if lane < 128 else 128 + lane
    where_b = lambda lane: 128 + lane if lane < 128 else 192 + lane
    for ix in range(count):
        sx, kx = (1, ix) if ix < modes else (-1, count - ix)
        for iy in range(count):
            sy, ky = (1, iy) if iy < modes else (-1, count - iy)
            re = ix * count + iy
            im = re + count * count
            sign[re, where_a(lanes[kx, ky])] += 1
            if kx and ky:
                sign[re, where_b(lanes[kx, modes + ky])] -= sx * sy
            if kx:
                sign[im, where_b(lanes[kx, ky])] -= sx
            if ky:
                sign[im, where_a(lanes[kx, modes + ky])] -= sy
    f32 = lambda a: np.asarray(a, np.float32)
    return dict(cos_u=f32(cos_u), sin_u=f32(sin_u), pq=f32(np.stack([p, q], axis=1)), trig_y=f32(trig_y),
                z_fwd=z_fwd, z_inv=z_inv, to_trig=sign.astype(BF16), to_modes=sign.T.astype(BF16))


def forward_rows(v, z_fwd_ref, zs_ref, ts_ref, side, pair):
    y = dot(z_fwd_ref[...], jnp.concatenate(split3(v), axis=0))
    size = y.shape[0] // 3
    y = y[:size] + (y[size:2 * size] + y[2 * size:])
    rows = slice(pair * size, (pair + 1) * size)
    if side == 0:
        zs_ref[rows, :] = y
        return
    first = zs_ref[rows, :]
    for part, v in enumerate((first + y, first - y)):
        for t, s in enumerate(split3(v)):
            ts_ref[part, t, rows, :] = s


def forward_xy(g, ts_ref, xy_ref, acc_ref):
    @pl.when(g == 0)
    def _():
        acc_ref[...] = jnp.zeros_like(acc_ref)

    for part in range(2):
        acc_ref[part] += dot6([ts_ref[part, t] for t in range(3)], [xy_ref[part, t, g] for t in range(3)])


def forward_flush(acc_ref, pq_ref, rows_ref, out_ref, width, trigs):
    p, q = pq_ref[0:1], pq_ref[1:2]
    even, odd = acc_ref[0], acc_ref[1]
    a = p * even - q * odd
    b = q * even + p * odd
    tail = a[:, 128:] + pltpu.roll(b[:, 128:], 64, 1)
    packed = jnp.concatenate([a[:, :128], b[:, :128], tail], axis=1)
    rows_ref[...] = packed.reshape(width, trigs, PACK)
    half = trigs // 2
    for t in range(trigs):
        out_ref[t % half, 0, (t // half) * width:(t // half + 1) * width, :] = rows_ref[:, t, :]


def forward_kernel(width, trigs, p_ref, q_ref, z_fwd_ref, xy_ref, pq_ref, out_ref, zs_ref, ts_ref, acc_ref, rows_ref):
    g = pl.program_id(1)
    count = p_ref.shape[1]
    for side, ref in enumerate((p_ref, q_ref)):
        order = range(count) if side == 0 else range(count - 1, -1, -1)
        for pair in range(width // 2):
            v = jnp.concatenate([ref[0, i, 2 * pair:2 * pair + 2].reshape(-1, ref.shape[4]) for i in order], axis=1)
            forward_rows(v, z_fwd_ref, zs_ref, ts_ref, side, pair)
    forward_xy(g, ts_ref, xy_ref, acc_ref)

    @pl.when(g == pl.num_programs(1) - 1)
    def _():
        forward_flush(acc_ref, pq_ref, rows_ref, out_ref, width, trigs)


def inverse_xy(g, coef_ref, pq_ref, rows_ref, gs_ref, xyt_ref, sp_ref, width, trigs):
    @pl.when(g == 0)
    def _():
        half = trigs // 2
        for t in range(trigs):
            rows_ref[:, t, :] = coef_ref[t % half, 0, (t // half) * width:(t // half + 1) * width, :]
        packed = rows_ref[...].reshape(width * trigs, PACK)
        p, q = pq_ref[0:1], pq_ref[1:2]
        tail = packed[:, 256:]
        a = jnp.concatenate([packed[:, :128], tail], axis=1)
        b = jnp.concatenate([packed[:, 128:256], pltpu.roll(tail, 64, 1)], axis=1)
        for part, v in enumerate((p * a + q * b, p * b - q * a)):
            hi, mid, lo = split3(v)
            for i, s in enumerate((hi, hi, hi, mid, mid, lo)):
                gs_ref[part, :, i * 128:(i + 1) * 128] = s[:, :128]
            hi, mid, lo = [s[:, 128:].astype(F32) for s in (hi, mid, lo)]
            tail = (hi + pltpu.roll(hi, 32, 1)) + (pltpu.roll(hi, 64, 1) + pltpu.roll(mid, 96, 1))
            gs_ref[part, :, 768:896] = tail.astype(BF16)
            gs_ref[part, :, 896:1024] = (mid + pltpu.roll(lo, 32, 1)).astype(BF16)

    for part in range(2):
        sp_ref[part] = dot(gs_ref[part], xyt_ref[part, g])


def layer_sides(loads, mix_ref, z_inv_ref, sp_ref, u_ref, width, trigs, grid_z, emit, mingle):
    ones = jnp.ones((16, LANES), BF16)
    tiles = grid_z // 8

    def pointwise(side, tile):
        y = dot(mix_ref[...], jnp.concatenate([six_rows(split3(loads[side](tile))), ones], axis=0))
        u_ref[side, :, tile * 8:(tile + 1) * 8, :] = y.reshape(width, 8, LANES)

    for tile in range(tiles):
        pointwise(0, tile)
    for side in range(2):
        first = 0 if not mingle else min(tiles, (width // 2 + 1) // 2)
        for tile in range(first, tiles if side == 1 else first):
            pointwise(1, tile)
        for pair in range(width // 2):
            rows = slice(pair * 2 * trigs, (pair + 1) * 2 * trigs)
            even, odd = sp_ref[0, rows, :], sp_ref[1, rows, :]
            y = dot(z_inv_ref[...], six_rows(split3(even + odd if side == 0 else even - odd)))
            if mingle and side == 0 and pair % 2 == 0 and pair // 2 < tiles:
                pointwise(1, pair // 2)
            emit(side, pair, gelu(y + u_ref[side, 2 * pair:2 * pair + 2].reshape(2 * grid_z, LANES)))


def middle_kernel(width, trigs, grid_z, p_ref, q_ref, coef_ref, mix_ref, z_inv_ref, z_fwd_ref, xy_ref, xyt_ref, pq_ref,
                  v_ref, out_ref, rows_ref, gs_ref, sp_ref, u_ref, zs_ref, ts_ref, acc_ref):
    g = pl.program_id(1)
    count = p_ref.shape[1]
    inverse_xy(g, coef_ref, pq_ref, rows_ref, gs_ref, xyt_ref, sp_ref, width, trigs)
    def load(ref, order, tile):
        return jnp.concatenate([ref[0, i, :, tile * 8:(tile + 1) * 8, :].reshape(8 * width, -1) for i in order], axis=1)

    def emit(side, pair, v):
        size = 2 * grid_z
        v_ref[0, 0, side, pair * size:(pair + 1) * size, :] = v
        forward_rows(v, z_fwd_ref, zs_ref, ts_ref, side, pair)

    loads = [functools.partial(load, p_ref, range(count)), functools.partial(load, q_ref, range(count - 1, -1, -1))]
    layer_sides(loads, mix_ref, z_inv_ref, sp_ref, u_ref, width, trigs, grid_z, emit, True)
    forward_xy(g, ts_ref, xy_ref, acc_ref)

    @pl.when(g == pl.num_programs(1) - 1)
    def _():
        forward_flush(acc_ref, pq_ref, rows_ref, out_ref, width, trigs)


def last_kernel(width, trigs, grid_z, v_ref, coef_ref, mix_ref, z_inv_ref, xyt_ref, pq_ref,
                out_ref, rows_ref, gs_ref, sp_ref, u_ref):
    g = pl.program_id(1)
    y_loc = out_ref.shape[4]
    count = LANES // y_loc
    inverse_xy(g, coef_ref, pq_ref, rows_ref, gs_ref, xyt_ref, sp_ref, width, trigs)
    def load(side, tile):
        v = v_ref[0, 0, side].reshape(width, grid_z, LANES)[:, tile * 8:(tile + 1) * 8, :]
        return v.reshape(width * 8, LANES)

    def emit(side, pair, v):
        for i in range(count):
            x = count * g + i if side == 0 else out_ref.shape[1] - 1 - count * g - i
            out_ref[0, x, 2 * pair:2 * pair + 2] = v[:, i * y_loc:(i + 1) * y_loc].reshape(2, grid_z, y_loc)

    loads = [functools.partial(load, side) for side in range(2)]
    layer_sides(loads, mix_ref, z_inv_ref, sp_ref, u_ref, width, trigs, grid_z, emit, False)


def mix_kernel(width, in_ref, re_ref, im_ref, to_modes_ref, to_trig_ref, out_ref, f_ref, t_ref):
    batch, rows, _ = in_ref.shape
    n = re_ref.shape[2]
    f_ref[...] = sum(dot(s, to_modes_ref[...]) for s in split3(in_ref[...].reshape(batch * rows, PACK))[::-1]).reshape(batch, rows, 2 * n)

    def one(b, carry):
        f_cos, f_sin = f_ref[b, :width, :], f_ref[b, width:, :]
        s_re = f_cos[:, :n] + f_sin[:, n:]
        s_im = f_cos[:, n:] - f_sin[:, :n]
        t_re = jnp.zeros((width, n), F32)
        t_im = jnp.zeros((width, n), F32)
        for c in range(width):
            w_re, w_im = re_ref[c], im_ref[c]
            a, d = s_re[c:c + 1], s_im[c:c + 1]
            t_re += a * w_re - d * w_im
            t_im += a * w_im + d * w_re
        t_ref[b, :width, :] = jnp.concatenate([t_re, t_im], axis=1)
        t_ref[b, width:, :] = jnp.concatenate([-t_im, t_re], axis=1)
        return carry

    lax.fori_loop(0, batch, one, 0)
    out = sum(dot(s, to_trig_ref[...]) for s in split3(t_ref[...].reshape(batch * rows, 2 * n))[::-1])
    out_ref[...] = out.reshape(batch, rows, PACK)


def weights_kernel(col_devs, re_ref, im_ref, *refs):
    outs, buf, sem = refs[:-2], refs[-2], refs[-1]
    kz = lax.axis_index('ys') * col_devs + lax.axis_index('xs')
    size = buf.shape[1]
    width, _, n = outs[0].shape
    copies = []
    for i in range(len(outs)):
        ref = re_ref if i % 2 == 0 else im_ref
        copies.append(pltpu.make_async_copy(ref.at[pl.ds(i // 2 * size, size), kz], buf.at[i], sem.at[i]))
        copies[-1].start()
    for i, out in enumerate(outs):
        copies[i].wait()
        for c in range(width):
            out[c] = buf[i, pl.ds(c, n, stride=width), 0, :].T


def tables_kernel(x_ref, y_ref, w_ref, bias_ref, spread_ref, pick_ref, xyt_ref, *mix_refs):
    groups = xyt_ref.shape[1]
    y_loc = y_ref.shape[1]
    count = LANES // y_loc
    for part in range(2):
        for g in range(groups):
            v = jnp.concatenate([x_ref[part, :, g * count + i:g * count + i + 1] * y_ref[...] for i in range(count)], axis=1)
            terms = split3(v)
            for i, t in enumerate((0, 1, 2, 0, 1, 0)):
                xyt_ref[part, g, i * 128:(i + 1) * 128, :] = terms[t][:128]
                xyt_ref[part, g, 768 + i * 32:768 + (i + 1) * 32, :] = terms[t][128:160]
            xyt_ref[part, g, 960:, :] = jnp.zeros((64, LANES), BF16)
    spread = spread_ref[...]
    for layer, mix_ref in enumerate(mix_refs):
        rows, columns = mix_ref.shape
        six = jnp.zeros((rows, columns), F32)
        for t, s in enumerate(split3(w_ref[layer])):
            by_row = lax.dot_general(spread, s, (((1,), (1,)), ((), ())), preferred_element_type=F32).astype(BF16)
            six += dot(by_row, pick_ref[t])
        row, column = [lax.broadcasted_iota(jnp.int32, (rows, columns), d) for d in range(2)]
        six = jnp.where((row - column) % 8 == 0, six, 0.0)
        for t, s in enumerate(split3(bias_ref[layer])):
            six = jnp.where(column == 6 * rows + t, dot(spread, jnp.broadcast_to(s, (s.shape[0], 128)))[:, :1], six)
        mix_ref[...] = six.astype(BF16)


def full(shape):
    return pl.BlockSpec(shape, lambda *_: (0,) * len(shape))


def params(mib, grid=2):
    return pltpu.CompilerParams(dimension_semantics=('arbitrary',) * grid, vmem_limit_bytes=mib * 2 ** 20)


def solution(mesh):
    row_devs = mesh.shape['ys']
    col_devs = mesh.shape['xs']

    def local_layers(field, spec_real, spec_imag, mix_weight, bias):
        batch, x_loc, y_loc, grid_z, width = field.shape
        layers = spec_real.shape[0]
        modes = spec_real.shape[3]
        trigs = 2 * modes
        rows = width * trigs
        count = LANES // y_loc
        groups = x_loc // (2 * count)
        t = tables(modes, x_loc * col_devs, y_loc * row_devs, grid_z, x_loc, y_loc, col_devs, row_devs)
        x_index = lax.axis_index('xs')
        y_index = lax.axis_index('ys')
        trig_y = lax.dynamic_index_in_dim(jnp.asarray(t['trig_y']), y_index, 0, keepdims=False)
        pq = lax.dynamic_index_in_dim(jnp.asarray(t['pq']), x_index, 0, keepdims=False)
        trig_x = jnp.stack([jnp.asarray(t['cos_u']), jnp.asarray(t['sin_u'])])
        xy = (trig_x[:, :, None, :] * trig_y[None, None]).reshape(2, groups, LANES, LANES)
        xy = jnp.stack(split_xla(xy), axis=1)
        z_fwd, z_inv = jnp.asarray(t['z_fwd']), jnp.asarray(t['z_inv'])
        to_modes, to_trig = jnp.asarray(t['to_modes']), jnp.asarray(t['to_trig'])
        trig_yt = lax.dynamic_index_in_dim(jnp.asarray(np.swapaxes(t['trig_y'], 1, 2)), y_index, 0, keepdims=False)
        trig_xt = jnp.asarray(np.swapaxes(np.stack([t['cos_u'], t['sin_u']]), 1, 2))
        spread_rows = np.kron(np.eye(width), np.ones((8, 1)))
        pick = np.zeros((3, width, 48 * width + 16))
        for i, term in enumerate((0, 1, 2, 0, 1, 0)):
            pick[term, :, i * 8 * width:(i + 1) * 8 * width] = spread_rows.T
        spread_rows, pick = jnp.asarray(spread_rows, BF16), jnp.asarray(pick, BF16)

        by_row = lambda w: jnp.transpose(w, (0, 1, 2, 4, 3, 5)).reshape(layers * trigs * trigs * width, modes, 1, width)
        own = pl.pallas_call(
            functools.partial(weights_kernel, col_devs), in_specs=[pl.BlockSpec(memory_space=pl.ANY)] * 2,
            out_shape=[jax.ShapeDtypeStruct((width, width, trigs * trigs), F32)] * (2 * layers),
            scratch_shapes=[pltpu.VMEM((2 * layers, trigs * trigs * width, 1, width), F32), pltpu.SemaphoreType.DMA((2 * layers,))],
            cost_estimate=pl.CostEstimate(flops=400000000, bytes_accessed=2 ** 24, transcendentals=0),
            compiler_params=pltpu.CompilerParams(vmem_limit_bytes=32 * 2 ** 20), name='weights')(by_row(spec_real), by_row(spec_imag))

        native = jnp.transpose(field, (0, 1, 4, 3, 2))
        xy_spec = full(xy.shape)
        packed_block = pl.BlockSpec((1, 1, 2, width * grid_z, LANES), lambda b, g: (b, g, 0, 0, 0))
        rows_scr = pltpu.VMEM((width, trigs, PACK), F32)
        zs_scr = pltpu.VMEM((rows, LANES), F32)
        ts_scr = pltpu.VMEM((2, 3, rows, LANES), BF16)
        acc_scr = pltpu.VMEM((2, rows, LANES), F32)
        gs_scr = pltpu.VMEM((2, rows, 4 * LANES), BF16)
        sp_scr = pltpu.VMEM((2, rows, LANES), F32)
        u_scr = pltpu.VMEM((2, width, grid_z, LANES), F32)

        half, part = batch // 2, batch // 4

        def field_blocks(first):
            shape = (1, count, width, grid_z, y_loc)
            return [pl.BlockSpec(shape, lambda b, g: (first + b, g, 0, 0, 0)),
                    pl.BlockSpec(shape, lambda b, g: (first + b, 2 * groups - 1 - g, 0, 0, 0))]

        def cost(us, n):
            return pl.CostEstimate(flops=int(us * n * 4e7), bytes_accessed=n * 13 * 2 ** 20, transcendentals=0)

        def ordered(kernel, after, specs, args, **settings):
            extra = len(after)
            return pl.pallas_call(lambda *refs: kernel(*refs[extra:]), in_specs=[pl.BlockSpec(memory_space=pl.ANY)] * extra + specs,
                                  **settings)(*after, *args)

        sums = jax.ShapeDtypeStruct((modes, half, 2 * width, PACK), F32)

        def sums_block(at):
            return pl.BlockSpec((modes, 1, 2 * width, PACK), lambda b, g: (0, at + b, 0, 0))

        def forward(first, n, at, into, after):
            return ordered(
                functools.partial(forward_kernel, width, trigs), after if into is None else [into] + after,
                field_blocks(first) + [full(z_fwd.shape), xy_spec, full(pq.shape)], [native, native, z_fwd, xy, pq],
                grid=(n, groups), out_specs=sums_block(at), out_shape=sums, scratch_shapes=[zs_scr, ts_scr, acc_scr, rows_scr],
                input_output_aliases={} if into is None else {0: 0},
                compiler_params=params(56), cost_estimate=cost(8, n), name='forward')

        def middle(first, n, at, coef, into, after):
            return ordered(
                functools.partial(middle_kernel, width, trigs, grid_z), after if into is None else [into] + after,
                field_blocks(first) + [sums_block(at), full(mix[0].shape), full(z_inv.shape), full(z_fwd.shape), xy_spec, full(xyt.shape), full(pq.shape)],
                [native, native, coef, mix[0], z_inv, z_fwd, xy, xyt, pq],
                grid=(n, groups), out_specs=[packed_block, sums_block(at)],
                out_shape=[jax.ShapeDtypeStruct((n, groups, 2, width * grid_z, LANES), F32), sums],
                scratch_shapes=[rows_scr, gs_scr, sp_scr, u_scr, zs_scr, ts_scr, acc_scr],
                input_output_aliases={} if into is None else {0: 1},
                compiler_params=params(60), cost_estimate=cost(20, n), name='middle')

        def last(first, n, at, v, coef, out, after):
            first_call = out is None
            return ordered(
                functools.partial(last_kernel, width, trigs, grid_z), after if first_call else [out] + after,
                [packed_block, sums_block(at), full(mix[1].shape), full(z_inv.shape), full(xyt.shape), full(pq.shape)],
                [v, coef, mix[1], z_inv, xyt, pq],
                grid=(n, groups), out_specs=pl.BlockSpec((1, x_loc, width, grid_z, y_loc), lambda b, g: (first + b, 0, 0, 0, 0)),
                out_shape=jax.ShapeDtypeStruct(native.shape, F32), scratch_shapes=[rows_scr, gs_scr, sp_scr, u_scr],
                input_output_aliases={} if first_call else {0: 0},
                compiler_params=params(60), cost_estimate=cost(12, n), name='last')

        def make_tables(after):
            args = [trig_xt, trig_yt, mix_weight, bias[:, :, None], spread_rows, pick]
            shapes = [(2, groups, 4 * LANES, LANES)] + [(8 * width, 48 * width + 16)] * layers
            return ordered(
                tables_kernel, after, [pl.BlockSpec(memory_space=pltpu.VMEM)] * len(args), args,
                out_shape=[jax.ShapeDtypeStruct(shape, BF16) for shape in shapes], cost_estimate=cost(1, 4),
                compiler_params=pltpu.CompilerParams(vmem_limit_bytes=32 * 2 ** 20), name='tables')

        def mixing(own_sum, layer, after):
            n = own_sum.shape[0]
            args = [own_sum, own[2 * layer], own[2 * layer + 1], to_modes, to_trig]
            return ordered(
                functools.partial(mix_kernel, width), after, [pl.BlockSpec(memory_space=pltpu.VMEM)] * len(args), args,
                out_shape=jax.ShapeDtypeStruct((n, 2 * width, PACK), F32),
                scratch_shapes=[pltpu.VMEM((n, 2 * width, 2 * trigs * trigs), F32)] * 2, cost_estimate=cost(0.5, n),
                compiler_params=pltpu.CompilerParams(vmem_limit_bytes=32 * 2 ** 20), name='mixing')

        def gather_sum(partial):
            return lax.psum_scatter(partial, ('ys', 'xs'), scatter_dimension=0, tiled=False)

        def spread(mixed):
            return lax.all_gather(mixed, ('ys', 'xs'), axis=0, tiled=False)

        sum_a = gather_sum(forward(0, half, 0, None, []))
        fwd_b = forward(half, part, 0, None, [])
        xyt, *mix = make_tables([fwd_b])
        mix_a = mixing(sum_a, 0, [mix[0]])
        coef_a = spread(mix_a)
        fwd_b = forward(half + part, part, part, fwd_b, [mix_a])
        sum_b = gather_sum(fwd_b)
        v_0, mid_a = middle(0, part, 0, coef_a, None, [fwd_b])
        mix_b = mixing(sum_b, 0, [mid_a])
        coef_b = spread(mix_b)
        v_1, mid_a = middle(part, part, part, coef_a, mid_a, [mix_b])
        sum_a = gather_sum(mid_a)
        v_2, mid_b = middle(half, part, 0, coef_b, None, [mid_a])
        mix_a = mixing(sum_a, 1, [mid_b])
        coef_a = spread(mix_a)
        v_3, mid_b = middle(half + part, part, part, coef_b, mid_b, [mix_a])
        sum_b = gather_sum(mid_b)
        out = last(0, part, 0, v_0, coef_a, None, [mid_b])
        mix_b = mixing(sum_b, 1, [out])
        coef_b = spread(mix_b)
        out = last(part, part, part, v_1, coef_a, out, [mix_b])
        out = last(half, part, 0, v_2, coef_b, out, [])
        out = last(half + part, part, part, v_3, coef_b, out, [])
        return jnp.transpose(out, (0, 1, 4, 3, 2))

    field_spec = P('data', 'xs', 'ys', None, None)
    return jax.shard_map(local_layers, mesh=mesh, in_specs=(field_spec, P(), P(), P(), P()), out_specs=field_spec, check_vma=False)
```

```python
import functools
import math

import jax
import jax.numpy as jnp
import numpy as np
from jax import lax
from jax.experimental import pallas as pl
from jax.experimental.pallas import tpu as pltpu
from jax.sharding import PartitionSpec as P

F32 = jnp.float32
BF16 = jnp.bfloat16
LANES = 256
PACK = 384


def split_xla(v):
    hi = lax.reduce_precision(v, 8, 7)
    rest = v - hi
    mid = lax.reduce_precision(rest, 8, 7)
    return hi.astype(BF16), mid.astype(BF16), (rest - mid).astype(BF16)


def split_np(v):
    v = np.asarray(v, np.float32)
    hi = v.astype(BF16)
    rest = v - hi.astype(np.float32)
    mid = rest.astype(BF16)
    return hi, mid, (rest - mid.astype(np.float32)).astype(BF16)


def split3(v):
    hi = v.astype(BF16)
    rest = v - hi.astype(F32)
    mid = rest.astype(BF16)
    return hi, mid, (rest - mid.astype(F32)).astype(BF16)


def dot(a, b):
    return jnp.dot(a, b, preferred_element_type=F32)


def dot6(a, b):
    return (dot(a[2], b[0]) + dot(a[1], b[1]) + dot(a[0], b[2])) + (dot(a[1], b[0]) + dot(a[0], b[1])) + dot(a[0], b[0])


def six_rows(s):
    return jnp.concatenate([s[0], s[0], s[0], s[1], s[1], s[2]], axis=0)


def six_cols(s, xp=jnp):
    return xp.concatenate([s[0], s[1], s[2], s[0], s[1], s[0]], axis=1)


def gelu(h):
    c = math.sqrt(2.0 / math.pi)
    return (0.5 * h) * (1.0 + jnp.tanh(h * (c + (c * 0.044715) * (h * h))))


def lane_map(modes):
    lanes = {}
    for k in range(modes):
        for j in range(2 * modes):
            lanes[k, j] = k * 2 * modes + j
    for k in range(modes):
        lanes[k, 2 * modes] = 128 + k
    for j in range(2 * modes + 1):
        lanes[modes, j] = 128 + modes + j
    return lanes


def tables(modes, grid_x, grid_y, grid_z, x_loc, y_loc, col_devs, row_devs):
    lanes = lane_map(modes)
    used = np.zeros(LANES)
    k_of = np.zeros(LANES)
    j_of = np.zeros(LANES, np.int64)
    for (k, j), lane in lanes.items():
        used[lane], k_of[lane], j_of[lane] = 1.0, k, j
    u = np.arange(x_loc // 2) - (x_loc - 1) / 2.0
    ang = 2 * np.pi * u[:, None] * k_of[None, :] / grid_x
    cos_u, sin_u = np.cos(ang) * used, np.sin(ang) * used
    centre = np.arange(col_devs) * x_loc + (x_loc - 1) / 2.0
    ang = 2 * np.pi * centre[:, None] * k_of[None, :] / grid_x
    p, q = np.cos(ang) * used, np.sin(ang) * used
    y = np.arange(grid_y)
    freq = np.where(j_of <= modes, j_of, j_of - modes)
    ang = 2 * np.pi * ((y[:, None] * freq[None, :]) % grid_y) / grid_y
    trig_y = (np.where(j_of <= modes, np.cos(ang), np.sin(ang)) * used).reshape(row_devs, y_loc, LANES)
    z = np.arange(grid_z)
    kz = np.arange(modes)
    ang = 2 * np.pi * ((z[:, None] * kz[None, :]) % grid_z) / grid_z
    trig_z = np.concatenate([np.cos(ang), np.sin(ang)], axis=1)
    weight = np.where(kz == 0, 1.0, 2.0) / (grid_x * grid_y * grid_z)
    inv_z = trig_z * np.concatenate([weight, weight])[None, :]
    fwd2 = split_np(np.kron(np.eye(2), trig_z.T))
    zero = np.zeros_like(fwd2[0])
    z_fwd = np.concatenate([
        np.concatenate([fwd2[0], fwd2[0], fwd2[0]], axis=1),
        np.concatenate([fwd2[1], fwd2[1], zero], axis=1),
        np.concatenate([fwd2[2], zero, zero], axis=1)], axis=0)
    z_inv = six_cols(split_np(np.kron(np.eye(2), inv_z)), np)
    count = 2 * modes
    sign = np.zeros((2 * count * count, PACK), np.float32)
    where_a = lambda lane: lane if lane < 128 else 128 + lane
    where_b = lambda lane: 128 + lane if lane < 128 else 192 + lane
    for ix in range(count):
        sx, kx = (1, ix) if ix < modes else (-1, count - ix)
        for iy in range(count):
            sy, ky = (1, iy) if iy < modes else (-1, count - iy)
            re = ix * count + iy
            im = re + count * count
            sign[re, where_a(lanes[kx, ky])] += 1
            if kx and ky:
                sign[re, where_b(lanes[kx, modes + ky])] -= sx * sy
            if kx:
                sign[im, where_b(lanes[kx, ky])] -= sx
            if ky:
                sign[im, where_a(lanes[kx, modes + ky])] -= sy
    f32 = lambda a: np.asarray(a, np.float32)
    return dict(cos_u=f32(cos_u), sin_u=f32(sin_u), pq=f32(np.stack([p, q], axis=1)), trig_y=f32(trig_y),
                z_fwd=z_fwd, z_inv=z_inv, to_trig=sign.astype(BF16), to_modes=sign.T.astype(BF16))


def forward_rows(v, z_fwd_ref, zs_ref, ts_ref, side, pair):
    y = dot(z_fwd_ref[...], jnp.concatenate(split3(v), axis=0))
    size = y.shape[0] // 3
    y = y[:size] + (y[size:2 * size] + y[2 * size:])
    rows = slice(pair * size, (pair + 1) * size)
    if side == 0:
        zs_ref[rows, :] = y
        return
    first = zs_ref[rows, :]
    for part, v in enumerate((first + y, first - y)):
        for t, s in enumerate(split3(v)):
            ts_ref[part, t, rows, :] = s


def forward_xy(g, ts_ref, xy_ref, acc_ref):
    @pl.when(g == 0)
    def _():
        acc_ref[...] = jnp.zeros_like(acc_ref)

    for part in range(2):
        acc_ref[part] += dot6([ts_ref[part, t] for t in range(3)], [xy_ref[part, t, g] for t in range(3)])


def forward_flush(acc_ref, pq_ref, rows_ref, out_ref, width, trigs):
    p, q = pq_ref[0:1], pq_ref[1:2]
    even, odd = acc_ref[0], acc_ref[1]
    a = p * even - q * odd
    b = q * even + p * odd
    tail = a[:, 128:] + pltpu.roll(b[:, 128:], 64, 1)
    packed = jnp.concatenate([a[:, :128], b[:, :128], tail], axis=1)
    rows_ref[...] = packed.reshape(width, trigs, PACK)
    half = trigs // 2
    for t in range(trigs):
        out_ref[t % half, 0, (t // half) * width:(t // half + 1) * width, :] = rows_ref[:, t, :]


def forward_kernel(width, trigs, p_ref, q_ref, z_fwd_ref, xy_ref, pq_ref, out_ref, zs_ref, ts_ref, acc_ref, rows_ref):
    g = pl.program_id(1)
    count = p_ref.shape[1]
    for side, ref in enumerate((p_ref, q_ref)):
        order = range(count) if side == 0 else range(count - 1, -1, -1)
        for pair in range(width // 2):
            v = jnp.concatenate([ref[0, i, 2 * pair:2 * pair + 2].reshape(-1, ref.shape[4]) for i in order], axis=1)
            forward_rows(v, z_fwd_ref, zs_ref, ts_ref, side, pair)
    forward_xy(g, ts_ref, xy_ref, acc_ref)

    @pl.when(g == pl.num_programs(1) - 1)
    def _():
        forward_flush(acc_ref, pq_ref, rows_ref, out_ref, width, trigs)


def inverse_xy(g, coef_ref, pq_ref, rows_ref, gs_ref, xyt_ref, sp_ref, width, trigs):
    @pl.when(g == 0)
    def _():
        half = trigs // 2
        for t in range(trigs):
            rows_ref[:, t, :] = coef_ref[t % half, 0, (t // half) * width:(t // half + 1) * width, :]
        packed = rows_ref[...].reshape(width * trigs, PACK)
        p, q = pq_ref[0:1], pq_ref[1:2]
        tail = packed[:, 256:]
        a = jnp.concatenate([packed[:, :128], tail], axis=1)
        b = jnp.concatenate([packed[:, 128:256], pltpu.roll(tail, 64, 1)], axis=1)
        for part, v in enumerate((p * a + q * b, p * b - q * a)):
            hi, mid, lo = split3(v)
            for i, s in enumerate((hi, hi, hi, mid, mid, lo)):
                gs_ref[part, :, i * 128:(i + 1) * 128] = s[:, :128]
            hi, mid, lo = [s[:, 128:].astype(F32) for s in (hi, mid, lo)]
            tail = (hi + pltpu.roll(hi, 32, 1)) + (pltpu.roll(hi, 64, 1) + pltpu.roll(mid, 96, 1))
            gs_ref[part, :, 768:896] = tail.astype(BF16)
            gs_ref[part, :, 896:1024] = (mid + pltpu.roll(lo, 32, 1)).astype(BF16)

    for part in range(2):
        sp_ref[part] = dot(gs_ref[part], xyt_ref[part, g])


def layer_sides(loads, mix_ref, z_inv_ref, sp_ref, u_ref, width, trigs, grid_z, emit, mingle):
    ones = jnp.ones((16, LANES), BF16)
    tiles = grid_z // 8

    def pointwise(side, tile):
        y = dot(mix_ref[...], jnp.concatenate([six_rows(split3(loads[side](tile))), ones], axis=0))
        u_ref[side, :, tile * 8:(tile + 1) * 8, :] = y.reshape(width, 8, LANES)

    for tile in range(tiles):
        pointwise(0, tile)
    for side in range(2):
        first = 0 if not mingle else min(tiles, (width // 2 + 1) // 2)
        for tile in range(first, tiles if side == 1 else first):
            pointwise(1, tile)
        for pair in range(width // 2):
            rows = slice(pair * 2 * trigs, (pair + 1) * 2 * trigs)
            even, odd = sp_ref[0, rows, :], sp_ref[1, rows, :]
            y = dot(z_inv_ref[...], six_rows(split3(even + odd if side == 0 else even - odd)))
            if mingle and side == 0 and pair % 2 == 0 and pair // 2 < tiles:
                pointwise(1, pair // 2)
            emit(side, pair, gelu(y + u_ref[side, 2 * pair:2 * pair + 2].reshape(2 * grid_z, LANES)))


def middle_kernel(width, trigs, grid_z, p_ref, q_ref, coef_ref, mix_ref, z_inv_ref, z_fwd_ref, xy_ref, xyt_ref, pq_ref,
                  v_ref, out_ref, rows_ref, gs_ref, sp_ref, u_ref, zs_ref, ts_ref, acc_ref):
    g = pl.program_id(1)
    count = p_ref.shape[1]
    inverse_xy(g, coef_ref, pq_ref, rows_ref, gs_ref, xyt_ref, sp_ref, width, trigs)
    def load(ref, order, tile):
        return jnp.concatenate([ref[0, i, :, tile * 8:(tile + 1) * 8, :].reshape(8 * width, -1) for i in order], axis=1)

    def emit(side, pair, v):
        size = 2 * grid_z
        v_ref[0, 0, side, pair * size:(pair + 1) * size, :] = v
        forward_rows(v, z_fwd_ref, zs_ref, ts_ref, side, pair)

    loads = [functools.partial(load, p_ref, range(count)), functools.partial(load, q_ref, range(count - 1, -1, -1))]
    layer_sides(loads, mix_ref, z_inv_ref, sp_ref, u_ref, width, trigs, grid_z, emit, True)
    forward_xy(g, ts_ref, xy_ref, acc_ref)

    @pl.when(g == pl.num_programs(1) - 1)
    def _():
        forward_flush(acc_ref, pq_ref, rows_ref, out_ref, width, trigs)


def last_kernel(width, trigs, grid_z, v_ref, coef_ref, mix_ref, z_inv_ref, xyt_ref, pq_ref,
                out_ref, rows_ref, gs_ref, sp_ref, u_ref):
    g = pl.program_id(1)
    y_loc = out_ref.shape[4]
    count = LANES // y_loc
    inverse_xy(g, coef_ref, pq_ref, rows_ref, gs_ref, xyt_ref, sp_ref, width, trigs)
    def load(side, tile):
        v = v_ref[0, 0, side].reshape(width, grid_z, LANES)[:, tile * 8:(tile + 1) * 8, :]
        return v.reshape(width * 8, LANES)

    def emit(side, pair, v):
        for i in range(count):
            x = count * g + i if side == 0 else out_ref.shape[1] - 1 - count * g - i
            out_ref[0, x, 2 * pair:2 * pair + 2] = v[:, i * y_loc:(i + 1) * y_loc].reshape(2, grid_z, y_loc)

    loads = [functools.partial(load, side) for side in range(2)]
    layer_sides(loads, mix_ref, z_inv_ref, sp_ref, u_ref, width, trigs, grid_z, emit, False)


def mix_kernel(width, in_ref, re_ref, im_ref, to_modes_ref, to_trig_ref, out_ref, f_ref, t_ref):
    batch, rows, _ = in_ref.shape
    n = re_ref.shape[2]
    f_ref[...] = sum(dot(s, to_modes_ref[...]) for s in split3(in_ref[...].reshape(batch * rows, PACK))[::-1]).reshape(batch, rows, 2 * n)

    def one(b, carry):
        f_cos, f_sin = f_ref[b, :width, :], f_ref[b, width:, :]
        s_re = f_cos[:, :n] + f_sin[:, n:]
        s_im = f_cos[:, n:] - f_sin[:, :n]
        t_re = jnp.zeros((width, n), F32)
        t_im = jnp.zeros((width, n), F32)
        for c in range(width):
            w_re, w_im = re_ref[c], im_ref[c]
            a, d = s_re[c:c + 1], s_im[c:c + 1]
            t_re += a * w_re - d * w_im
            t_im += a * w_im + d * w_re
        t_ref[b, :width, :] = jnp.concatenate([t_re, t_im], axis=1)
        t_ref[b, width:, :] = jnp.concatenate([-t_im, t_re], axis=1)
        return carry

    lax.fori_loop(0, batch, one, 0)
    out = sum(dot(s, to_trig_ref[...]) for s in split3(t_ref[...].reshape(batch * rows, 2 * n))[::-1])
    out_ref[...] = out.reshape(batch, rows, PACK)


def weights_kernel(col_devs, re_ref, im_ref, *refs):
    outs, buf, sem = refs[:-2], refs[-2], refs[-1]
    kz = lax.axis_index('ys') * col_devs + lax.axis_index('xs')
    size = buf.shape[1]
    width, _, n = outs[0].shape
    copies = []
    for i in range(len(outs)):
        ref = re_ref if i % 2 == 0 else im_ref
        copies.append(pltpu.make_async_copy(ref.at[pl.ds(i // 2 * size, size), kz], buf.at[i], sem.at[i]))
        copies[-1].start()
    for i, out in enumerate(outs):
        copies[i].wait()
        for c in range(width):
            out[c] = buf[i, pl.ds(c, n, stride=width), 0, :].T


def tables_kernel(x_ref, y_ref, w_ref, bias_ref, spread_ref, pick_ref, xyt_ref, *mix_refs):
    groups = xyt_ref.shape[1]
    y_loc = y_ref.shape[1]
    count = LANES // y_loc
    for part in range(2):
        for g in range(groups):
            v = jnp.concatenate([x_ref[part, :, g * count + i:g * count + i + 1] * y_ref[...] for i in range(count)], axis=1)
            terms = split3(v)
            for i, t in enumerate((0, 1, 2, 0, 1, 0)):
                xyt_ref[part, g, i * 128:(i + 1) * 128, :] = terms[t][:128]
                xyt_ref[part, g, 768 + i * 32:768 + (i + 1) * 32, :] = terms[t][128:160]
            xyt_ref[part, g, 960:, :] = jnp.zeros((64, LANES), BF16)
    spread = spread_ref[...]
    for layer, mix_ref in enumerate(mix_refs):
        rows, columns = mix_ref.shape
        six = jnp.zeros((rows, columns), F32)
        for t, s in enumerate(split3(w_ref[layer])):
            by_row = lax.dot_general(spread, s, (((1,), (1,)), ((), ())), preferred_element_type=F32).astype(BF16)
            six += dot(by_row, pick_ref[t])
        row, column = [lax.broadcasted_iota(jnp.int32, (rows, columns), d) for d in range(2)]
        six = jnp.where((row - column) % 8 == 0, six, 0.0)
        for t, s in enumerate(split3(bias_ref[layer])):
            six = jnp.where(column == 6 * rows + t, dot(spread, jnp.broadcast_to(s, (s.shape[0], 128)))[:, :1], six)
        mix_ref[...] = six.astype(BF16)


def full(shape):
    return pl.BlockSpec(shape, lambda *_: (0,) * len(shape))


def params(mib, grid=2):
    return pltpu.CompilerParams(dimension_semantics=('arbitrary',) * grid, vmem_limit_bytes=mib * 2 ** 20)


def solution(mesh):
    row_devs = mesh.shape['ys']
    col_devs = mesh.shape['xs']

    def local_layers(field, spec_real, spec_imag, mix_weight, bias):
        batch, x_loc, y_loc, grid_z, width = field.shape
        layers = spec_real.shape[0]
        modes = spec_real.shape[3]
        trigs = 2 * modes
        rows = width * trigs
        count = LANES // y_loc
        groups = x_loc // (2 * count)
        t = tables(modes, x_loc * col_devs, y_loc * row_devs, grid_z, x_loc, y_loc, col_devs, row_devs)
        x_index = lax.axis_index('xs')
        y_index = lax.axis_index('ys')
        trig_y = lax.dynamic_index_in_dim(jnp.asarray(t['trig_y']), y_index, 0, keepdims=False)
        pq = lax.dynamic_index_in_dim(jnp.asarray(t['pq']), x_index, 0, keepdims=False)
        trig_x = jnp.stack([jnp.asarray(t['cos_u']), jnp.asarray(t['sin_u'])])
        xy = (trig_x[:, :, None, :] * trig_y[None, None]).reshape(2, groups, LANES, LANES)
        xy = jnp.stack(split_xla(xy), axis=1)
        z_fwd, z_inv = jnp.asarray(t['z_fwd']), jnp.asarray(t['z_inv'])
        to_modes, to_trig = jnp.asarray(t['to_modes']), jnp.asarray(t['to_trig'])
        trig_yt = lax.dynamic_index_in_dim(jnp.asarray(np.swapaxes(t['trig_y'], 1, 2)), y_index, 0, keepdims=False)
        trig_xt = jnp.asarray(np.swapaxes(np.stack([t['cos_u'], t['sin_u']]), 1, 2))
        spread_rows = np.kron(np.eye(width), np.ones((8, 1)))
        pick = np.zeros((3, width, 48 * width + 16))
        for i, term in enumerate((0, 1, 2, 0, 1, 0)):
            pick[term, :, i * 8 * width:(i + 1) * 8 * width] = spread_rows.T
        spread_rows, pick = jnp.asarray(spread_rows, BF16), jnp.asarray(pick, BF16)

        by_row = lambda w: jnp.transpose(w, (0, 1, 2, 4, 3, 5)).reshape(layers * trigs * trigs * width, modes, 1, width)
        own = pl.pallas_call(
            functools.partial(weights_kernel, col_devs), in_specs=[pl.BlockSpec(memory_space=pl.ANY)] * 2,
            out_shape=[jax.ShapeDtypeStruct((width, width, trigs * trigs), F32)] * (2 * layers),
            scratch_shapes=[pltpu.VMEM((2 * layers, trigs * trigs * width, 1, width), F32), pltpu.SemaphoreType.DMA((2 * layers,))],
            cost_estimate=pl.CostEstimate(flops=400000000, bytes_accessed=2 ** 24, transcendentals=0),
            compiler_params=pltpu.CompilerParams(vmem_limit_bytes=32 * 2 ** 20), name='weights')(by_row(spec_real), by_row(spec_imag))

        native = jnp.transpose(field, (0, 1, 4, 3, 2))
        xy_spec = full(xy.shape)
        packed_at = lambda at: pl.BlockSpec((1, 1, 2, width * grid_z, LANES), lambda b, g: (at + b, g, 0, 0, 0))
        packed_block = pl.BlockSpec((1, 1, 2, width * grid_z, LANES), lambda b, g: (b, g, 0, 0, 0))
        rows_scr = pltpu.VMEM((width, trigs, PACK), F32)
        zs_scr = pltpu.VMEM((rows, LANES), F32)
        ts_scr = pltpu.VMEM((2, 3, rows, LANES), BF16)
        acc_scr = pltpu.VMEM((2, rows, LANES), F32)
        gs_scr = pltpu.VMEM((2, rows, 4 * LANES), BF16)
        sp_scr = pltpu.VMEM((2, rows, LANES), F32)
        u_scr = pltpu.VMEM((2, width, grid_z, LANES), F32)

        half, part = batch // 2, batch // 4

        def field_blocks(first):
            shape = (1, count, width, grid_z, y_loc)
            return [pl.BlockSpec(shape, lambda b, g: (first + b, g, 0, 0, 0)),
                    pl.BlockSpec(shape, lambda b, g: (first + b, 2 * groups - 1 - g, 0, 0, 0))]

        def cost(us, n):
            return pl.CostEstimate(flops=int(us * n * 4e7), bytes_accessed=n * 13 * 2 ** 20, transcendentals=0)

        def ordered(kernel, after, specs, args, **settings):
            extra = len(after)
            return pl.pallas_call(lambda *refs: kernel(*refs[extra:]), in_specs=[pl.BlockSpec(memory_space=pl.ANY)] * extra + specs,
                                  **settings)(*after, *args)

        sums = jax.ShapeDtypeStruct((modes, half, 2 * width, PACK), F32)

        def sums_block(at):
            return pl.BlockSpec((modes, 1, 2 * width, PACK), lambda b, g: (0, at + b, 0, 0))

        def forward(first, n, at, into, after):
            return ordered(
                functools.partial(forward_kernel, width, trigs), after if into is None else [into] + after,
                field_blocks(first) + [full(z_fwd.shape), xy_spec, full(pq.shape)], [native, native, z_fwd, xy, pq],
                grid=(n, groups), out_specs=sums_block(at), out_shape=sums, scratch_shapes=[zs_scr, ts_scr, acc_scr, rows_scr],
                input_output_aliases={} if into is None else {0: 0},
                compiler_params=params(56), cost_estimate=cost(8, n), name='forward')

        def middle(first, n, at, coef, into, into_v, size_v, after):
            return ordered(
                functools.partial(middle_kernel, width, trigs, grid_z), [a for a in (into, into_v) if a is not None] + after,
                field_blocks(first) + [sums_block(at), full(mix[0].shape), full(z_inv.shape), full(z_fwd.shape), xy_spec, full(xyt.shape), full(pq.shape)],
                [native, native, coef, mix[0], z_inv, z_fwd, xy, xyt, pq],
                grid=(n, groups), out_specs=[packed_block if into_v is None else packed_at(at), sums_block(at)],
                out_shape=[jax.ShapeDtypeStruct((size_v, groups, 2, width * grid_z, LANES), F32), sums],
                scratch_shapes=[rows_scr, gs_scr, sp_scr, u_scr, zs_scr, ts_scr, acc_scr],
                input_output_aliases={} if into is None else {0: 1} if into_v is None else {0: 1, 1: 0},
                compiler_params=params(60), cost_estimate=cost(20, n), name='middle')

        def last(first, n, at, v, coef, out, after):
            first_call = out is None
            return ordered(
                functools.partial(last_kernel, width, trigs, grid_z), after if first_call else [out] + after,
                [packed_block, sums_block(at), full(mix[1].shape), full(z_inv.shape), full(xyt.shape), full(pq.shape)],
                [v, coef, mix[1], z_inv, xyt, pq],
                grid=(n, groups), out_specs=pl.BlockSpec((1, x_loc, width, grid_z, y_loc), lambda b, g: (first + b, 0, 0, 0, 0)),
                out_shape=jax.ShapeDtypeStruct(native.shape, F32), scratch_shapes=[rows_scr, gs_scr, sp_scr, u_scr],
                input_output_aliases={} if first_call else {0: 0},
                compiler_params=params(60), cost_estimate=cost(12, n), name='last')

        def make_tables(after):
            args = [trig_xt, trig_yt, mix_weight, bias[:, :, None], spread_rows, pick]
            shapes = [(2, groups, 4 * LANES, LANES)] + [(8 * width, 48 * width + 16)] * layers
            return ordered(
                tables_kernel, after, [pl.BlockSpec(memory_space=pltpu.VMEM)] * len(args), args,
                out_shape=[jax.ShapeDtypeStruct(shape, BF16) for shape in shapes], cost_estimate=cost(1, 4),
                compiler_params=pltpu.CompilerParams(vmem_limit_bytes=32 * 2 ** 20), name='tables')

        def mixing(own_sum, layer, after):
            n = own_sum.shape[0]
            args = [own_sum, own[2 * layer], own[2 * layer + 1], to_modes, to_trig]
            return ordered(
                functools.partial(mix_kernel, width), after, [pl.BlockSpec(memory_space=pltpu.VMEM)] * len(args), args,
                out_shape=jax.ShapeDtypeStruct((n, 2 * width, PACK), F32),
                scratch_shapes=[pltpu.VMEM((n, 2 * width, 2 * trigs * trigs), F32)] * 2, cost_estimate=cost(0.5, n),
                compiler_params=pltpu.CompilerParams(vmem_limit_bytes=32 * 2 ** 20), name='mixing')

        def gather_sum(partial):
            return lax.psum_scatter(partial, ('ys', 'xs'), scatter_dimension=0, tiled=False)

        def spread(mixed):
            return lax.all_gather(mixed, ('ys', 'xs'), axis=0, tiled=False)

        sum_a = gather_sum(forward(0, half, 0, None, []))
        fwd_b = forward(half, part, 0, None, [])
        xyt, *mix = make_tables([fwd_b])
        mix_a = mixing(sum_a, 0, [mix[0]])
        coef_a = spread(mix_a)
        fwd_b = forward(half + part, part, part, fwd_b, [mix_a])
        sum_b = gather_sum(fwd_b)
        v_0, mid_a = middle(0, part, 0, coef_a, None, None, part, [fwd_b])
        mix_b = mixing(sum_b, 0, [mid_a])
        coef_b = spread(mix_b)
        v_1, mid_a = middle(part, part, part, coef_a, mid_a, None, part, [mix_b])
        sum_a = gather_sum(mid_a)
        v_b, mid_b = middle(half, part, 0, coef_b, None, None, half, [mid_a])
        mix_a = mixing(sum_a, 1, [mid_b])
        coef_a = spread(mix_a)
        v_b, mid_b = middle(half + part, part, part, coef_b, mid_b, v_b, half, [mix_a])
        sum_b = gather_sum(mid_b)
        out = last(0, part, 0, v_0, coef_a, None, [mid_b])
        mix_b = mixing(sum_b, 1, [out])
        coef_b = spread(mix_b)
        out = last(part, part, part, v_1, coef_a, out, [mix_b])
        out = last(half, half, 0, v_b, coef_b, out, [])
        return jnp.transpose(out, (0, 1, 4, 3, 2))

    field_spec = P('data', 'xs', 'ys', None, None)
    return jax.shard_map(local_layers, mesh=mesh, in_specs=(field_spec, P(), P(), P(), P()), out_specs=field_spec, check_vma=False)
```
